8 devices in a mesh: dp: 1 (over z), cx: 2 (over y), cy: 4 (over x, core).
Axes of the slice: x: 2, y: 2, z: 1, core: 2. Of those that a mesh axis runs over, the one named last changes fastest.
Arguments:
- x: bfloat16 [1, 2048, 1536], P('dp', ('cx', 'cy'))
- w_qkv: bfloat16 [1536, 4608], replicated
- w_o: bfloat16 [12, 128, 1536], replicated
Outputs:
- output: bfloat16 [1, 2048, 1536], P('dp', ('cx', 'cy'))
All inputs are finite; a program needn't handle non-finite values.
Results may differ from the reference program's by a relative error of at most 0.00801888.
Values are sent between devices in bfloat16 or wider.
A program may use at most 1 GiB of HBM per device.

```python
import math
import jax
import jax.numpy as jnp
from jax import lax

SEQ_LEN = 2048
NUM_HEADS = 12
HEAD_DIM = 128


def setup_inputs(seed: int = 0, part: int = 0) -> dict:
    model_width = NUM_HEADS * HEAD_DIM
    base_key = jax.random.key(seed)
    token_key = jax.random.fold_in(jax.random.fold_in(base_key, part), 1)
    qkv_key = jax.random.fold_in(base_key, 2)
    out_key = jax.random.fold_in(base_key, 3)
    logit_std = math.sqrt(max(math.log(SEQ_LEN / 20.0), 2.0))
    qk_gain = math.sqrt(logit_std)
    col_gain = jnp.concatenate([jnp.full((2 * model_width,), qk_gain, jnp.float32), jnp.ones((model_width,), jnp.float32)])
    tokens = jax.random.normal(token_key, (1, SEQ_LEN, model_width), jnp.float32)
    w_qkv = jax.random.normal(qkv_key, (model_width, 3 * model_width), jnp.float32) * (model_width ** -0.5) * col_gain
    w_out = jax.random.normal(out_key, (NUM_HEADS, HEAD_DIM, model_width), jnp.float32) * (2.5 * model_width ** -0.5)
    return {"x": tokens.astype(jnp.bfloat16), "w_qkv": w_qkv.astype(jnp.bfloat16), "w_o": w_out.astype(jnp.bfloat16)}


def reference(x, w_qkv, w_o):
    model_width = NUM_HEADS * HEAD_DIM
    q_block = math.gcd(SEQ_LEN, 256)
    n_blocks = SEQ_LEN // q_block
    inv_sqrt = 1.0 / math.sqrt(HEAD_DIM)
    qkv_rows = jnp.dot(x[0], w_qkv, preferred_element_type=jnp.float32).astype(jnp.bfloat16)
    qkv_rows = jnp.transpose(qkv_rows.reshape(SEQ_LEN, 3, NUM_HEADS, HEAD_DIM), (1, 2, 0, 3))

    def head_attend(head_args):
        q_head, k_head, v_head = head_args
        k_full = k_head.astype(jnp.float32)
        v_full = v_head.astype(jnp.float32)
        q_blocks = q_head.astype(jnp.float32).reshape(n_blocks, q_block, HEAD_DIM)

        def block_attend(q_rows):
            logits = jnp.dot(q_rows, k_full.T, preferred_element_type=jnp.float32) * inv_sqrt
            row_max = jnp.max(logits, axis=-1, keepdims=True)
            weights = jnp.exp(logits - row_max)
            row_sum = jnp.sum(weights, axis=-1, keepdims=True)
            return jnp.dot(weights, v_full, preferred_element_type=jnp.float32) / row_sum

        return lax.map(block_attend, q_blocks).reshape(SEQ_LEN, HEAD_DIM)

    attn_rows = lax.map(head_attend, (qkv_rows[0], qkv_rows[1], qkv_rows[2]))
    attn_rows = jnp.transpose(attn_rows, (1, 0, 2)).reshape(SEQ_LEN, model_width).astype(jnp.bfloat16)
    result = jnp.dot(attn_rows, w_o.reshape(model_width, model_width), preferred_element_type=jnp.float32)
    return result.astype(jnp.bfloat16)[None]
```

```python
import functools
import math

import jax
import jax.numpy as jnp
from jax import lax
from jax.experimental import pallas as pl
from jax.experimental.pallas import tpu as pltpu
from jax.sharding import PartitionSpec as P

MESH = pl.DeviceIdType.MESH
BF16, F32 = jnp.bfloat16, jnp.float32
HEAD = 128


def kernel(x_hbm, wqkv_hbm, wo_hbm, y_ref,
           xbuf, wq, wk, wv, wo, qt, kbuf, vbuf, acc, mrow, lrow, osend, oown, oother, yacc,
           w_sem, own_sem, pair_sem, send_sem, fwd_sem, relay_sem, osend_sem,
           precv_sem, recv_sem, orecv_sem):
    tok, width = x_hbm.shape
    half = width // 2
    nh = half // HEAD
    quarter = tok // 4
    scale = math.log2(math.e) / math.sqrt(HEAD)

    dp, cx, cy = lax.axis_index("dp"), lax.axis_index("cx"), lax.axis_index("cy")
    core = lax.rem(cy, 2)
    partner = (dp, cx, cy + 1 - 2 * core)
    xnbr = (dp, cx, lax.rem(cy + 2, 4))
    ynbr = (dp, 1 - cx, cy)

    def wcopy(i, dst):
        cols = pl.ds(pl.multiple_of(i * width + core * half, HEAD), half)
        return pltpu.make_async_copy(wqkv_hbm.at[:, cols], dst, w_sem.at[i])

    xload = pltpu.make_async_copy(x_hbm, xbuf.at[0], own_sem)
    xload.start()
    wq_copy, wk_copy, wv_copy = wcopy(0, wq), wcopy(1, wk), wcopy(2, wv)
    wo_copy = pltpu.make_async_copy(wo_hbm, wo, w_sem.at[3])
    wq_copy.start()
    wk_copy.start()
    wv_copy.start()

    barrier = pltpu.get_barrier_semaphore()
    for nbr in (partner, xnbr, ynbr):
        pl.semaphore_signal(barrier, inc=1, device_id=nbr, device_id_type=MESH)
    pl.semaphore_wait(barrier, 3)

    def remote(src, dst, ssem, rsem, dev):
        return pltpu.make_async_remote_copy(src_ref=src, dst_ref=dst, send_sem=ssem, recv_sem=rsem,
                                            device_id=dev, device_id_type=MESH)

    def part(step, q):
        return xbuf.at[step, pl.ds(q * quarter, quarter), :]

    def own_rows(i):
        return xbuf.at[0, pl.ds(i * quarter, quarter), :]

    def xsend(i):
        return remote(own_rows((i + 2) % 4), part(2 + i, 0), send_sem.at[0, i], recv_sem.at[2 + i, 0], xnbr)

    def ysend(i):
        return remote(own_rows(i), part(2 + i, 2), send_sem.at[1, i], recv_sem.at[2 + i, 2], ynbr)

    pair_copy = remote(xbuf.at[0], xbuf.at[1], pair_sem, precv_sem, partner)

    def fwd(step, q):
        return remote(part(step, q), part(step, q + 1), fwd_sem.at[step, q // 2], recv_sem.at[step, q + 1], partner)

    def xrelay(step):
        return remote(part(step, 2), part(step + 4, 0), relay_sem.at[0, step], recv_sem.at[step + 4, 0], xnbr)

    def yrelay(step):
        return remote(part(step, 0), part(step + 4, 2), relay_sem.at[1, step], recv_sem.at[step + 4, 2], ynbr)

    def await_recv(step, q):
        remote(part(step, q), part(step, q), fwd_sem.at[step, 0], recv_sem.at[step, q], partner).wait_recv()

    xload.wait()
    for i in range(4):
        xsend(i).start()
        ysend(i).start()
        if i == 0:
            pair_copy.start()
    wo_copy.start()

    def dot(a, b):
        return jnp.dot(a, b, preferred_element_type=F32)

    def dot_t(a, b):
        return lax.dot_general(a, b, (((0,), (0,)), ((), ())), preferred_element_type=F32)

    def project_q(step):
        q = dot(xbuf[step], wq[...])
        for h in range(nh):
            qt[h, :, step * tok:(step + 1) * tok] = q[:, h * HEAD:(h + 1) * HEAD].T.astype(BF16)

    def project_kv(step):
        xs = xbuf[step]
        kbuf[...] = dot(xs, wk[...]).astype(BF16)
        vbuf[...] = dot(xs, wv[...]).astype(BF16)

    def attend():
        def logits(h):
            return dot(kbuf[:, h * HEAD:(h + 1) * HEAD], qt[h])

        s = logits(0)
        for h in range(nh):
            s_next = logits(h + 1) if h + 1 < nh else None
            m_old = mrow[h]
            m_new = jnp.maximum(m_old, jnp.max(s, axis=0, keepdims=True))
            p = jnp.exp2((s - m_new) * scale)
            a = jnp.exp2((m_old - m_new) * scale)
            lrow[h] = lrow[h] * a + jnp.sum(p, axis=0, keepdims=True)
            mrow[h] = m_new
            acc[h] = acc[h] * a + dot_t(vbuf[:, h * HEAD:(h + 1) * HEAD], p.astype(BF16))
            s = s_next

    acc[...] = jnp.zeros_like(acc)
    lrow[...] = jnp.zeros_like(lrow)
    mrow[...] = jnp.full(mrow.shape, -jnp.inf, F32)

    wq_copy.wait()
    project_q(0)
    wk_copy.wait()
    wv_copy.wait()
    project_kv(0)
    pair_copy.wait_recv()
    project_q(1)
    attend()
    project_kv(1)

    def body(step, carry):
        await_recv(step, 0)
        await_recv(step, 2)
        fwd(step, 0).start()
        fwd(step, 2).start()

        @pl.when(step < 4)
        def _():
            xrelay(step).start()
            yrelay(step).start()

        attend()
        await_recv(step, 1)
        await_recv(step, 3)
        project_kv(step)
        return carry

    lax.fori_loop(2, 8, body, 0)
    attend()

    def osend_copy(h):
        return remote(osend.at[h], oother.at[h], osend_sem.at[h], orecv_sem.at[h], partner)

    for h in range(nh):
        o = (acc[h] / lrow[h]).astype(BF16)
        oown[h * HEAD:(h + 1) * HEAD, :] = o[:, :tok]
        osend[h] = o[:, tok:]
    for h in range(nh):
        osend_copy(h).start()
    wo_copy.wait()
    own_rows_w = pl.ds(pl.multiple_of(core * half, HEAD), half)
    other_rows_w = pl.ds(pl.multiple_of((1 - core) * half, HEAD), half)
    yacc[...] = dot_t(oown[...], wo[own_rows_w, :])
    for h in range(nh):
        osend_copy(h).wait_recv()
    y_ref[...] = (yacc[...] + dot_t(oother[...].reshape(half, tok), wo[other_rows_w, :])).astype(BF16)

    pair_copy.wait_send()
    for i in range(4):
        xsend(i).wait_send()
        ysend(i).wait_send()
    for step in range(2, 8):
        fwd(step, 0).wait_send()
        fwd(step, 2).wait_send()
    for step in range(2, 4):
        xrelay(step).wait_send()
        yrelay(step).wait_send()
    for h in range(nh):
        osend_copy(h).wait_send()


def solution(mesh):
    def block(x, w_qkv, w_o):
        tok, width = x.shape[1], x.shape[2]
        half = width // 2
        nh = half // HEAD
        any_spec = pl.BlockSpec(memory_space=pl.ANY)
        dma = pltpu.SemaphoreType.DMA
        y = pl.pallas_call(
            kernel,
            out_shape=jax.ShapeDtypeStruct((tok, width), BF16),
            in_specs=[any_spec] * 3,
            out_specs=pl.BlockSpec(memory_space=pltpu.VMEM),
            scratch_shapes=[
                pltpu.VMEM((8, tok, width), BF16),
                pltpu.VMEM((width, half), BF16),
                pltpu.VMEM((width, half), BF16),
                pltpu.VMEM((width, half), BF16),
                pltpu.VMEM((width, width), BF16),
                pltpu.VMEM((nh, HEAD, 2 * tok), BF16),
                pltpu.VMEM((tok, half), BF16),
                pltpu.VMEM((tok, half), BF16),
                pltpu.VMEM((nh, HEAD, 2 * tok), F32),
                pltpu.VMEM((nh, 1, 2 * tok), F32),
                pltpu.VMEM((nh, 1, 2 * tok), F32),
                pltpu.VMEM((nh, HEAD, tok), BF16),
                pltpu.VMEM((half, tok), BF16),
                pltpu.VMEM((nh, HEAD, tok), BF16),
                pltpu.VMEM((tok, width), F32),
                dma((4,)), dma(()), dma(()), dma((2, 4)), dma((8, 2)), dma((2, 4)), dma((nh,)),
                dma(()), dma((8, 4)), dma((nh,)),
            ],
            compiler_params=pltpu.CompilerParams(
                collective_id=0, has_side_effects=True, vmem_limit_bytes=60 * 1024 * 1024),
            name="gather_attend",
        )(x[0], w_qkv, w_o.reshape(width, width))
        return y[None]

    return jax.shard_map(
        block, mesh=mesh,
        in_specs=(P("dp", ("cx", "cy"), None), P(None, None), P(None, None, None)),
        out_specs=P("dp", ("cx", "cy"), None), check_vma=False)
```

```python
import functools
import math

import jax
import jax.numpy as jnp
from jax import lax
from jax.experimental import pallas as pl
from jax.experimental.pallas import tpu as pltpu
from jax.sharding import PartitionSpec as P

MESH = pl.DeviceIdType.MESH
BF16, F32 = jnp.bfloat16, jnp.float32
HEAD = 128


def kernel(x_hbm, wqkv_hbm, wo_hbm, y_ref,
           xbuf, wq, wk, wv, wo, qt, kbuf, vbuf, acc, mrow, lrow, osend, oown, oother, yacc,
           w_sem, own_sem, pair_sem, send_sem, fwd_sem, relay_sem, osend_sem,
           precv_sem, recv_sem, orecv_sem):
    tok, width = x_hbm.shape
    half = width // 2
    nh = half // HEAD
    quarter = tok // 4
    scale = math.log2(math.e) / math.sqrt(HEAD)

    dp, cx, cy = lax.axis_index("dp"), lax.axis_index("cx"), lax.axis_index("cy")
    core = lax.rem(cy, 2)
    partner = (dp, cx, cy + 1 - 2 * core)
    xnbr = (dp, cx, lax.rem(cy + 2, 4))
    ynbr = (dp, 1 - cx, cy)

    def wcopy(i, dst):
        cols = pl.ds(pl.multiple_of(i * width + core * half, HEAD), half)
        return pltpu.make_async_copy(wqkv_hbm.at[:, cols], dst, w_sem.at[i])

    xload = pltpu.make_async_copy(x_hbm, xbuf.at[0], own_sem)
    wq_copy, wk_copy, wv_copy = wcopy(0, wq), wcopy(1, wk), wcopy(2, wv)
    wo_copy = pltpu.make_async_copy(wo_hbm, wo, w_sem.at[3])
    xload.start()

    barrier = pltpu.get_barrier_semaphore()
    for nbr in (partner, xnbr, ynbr):
        pl.semaphore_signal(barrier, inc=1, device_id=nbr, device_id_type=MESH)
    xload.wait()
    wq_copy.start()
    wk_copy.start()
    wv_copy.start()
    pl.semaphore_wait(barrier, 3)

    def remote(src, dst, ssem, rsem, dev):
        return pltpu.make_async_remote_copy(src_ref=src, dst_ref=dst, send_sem=ssem, recv_sem=rsem,
                                            device_id=dev, device_id_type=MESH)

    def part(step, q, sub=None):
        if sub is None:
            return xbuf.at[step, pl.ds(q * quarter, quarter), :]
        return xbuf.at[step, pl.ds(sub * 2 * quarter + q * (quarter // 2), quarter // 2), :]

    def own_rows(i):
        return xbuf.at[0, pl.ds(i * quarter, quarter), :]

    def xsend(i):
        return remote(own_rows((i + 2) % 4), part(2 + i, 0), send_sem.at[0, i], recv_sem.at[2 + i, 0], xnbr)

    def ysend(i):
        return remote(own_rows(i), part(2 + i, 2), send_sem.at[1, i], recv_sem.at[2 + i, 2], ynbr)

    pair_copy = remote(xbuf.at[0], xbuf.at[1], pair_sem, precv_sem, partner)

    def sem_of(step, sub):
        return step if not sub else step + sub

    def fwd(step, q, sub=None):
        n = sem_of(step, sub)
        return remote(part(step, q, sub), part(step, q + 1, sub), fwd_sem.at[n, q // 2], recv_sem.at[n, q + 1], partner)

    def relay(q, step, sub=None):
        n = sem_of(step + 4, sub)
        rows = pl.ds(q * quarter + (sub or 0) * (quarter // 2), quarter if sub is None else quarter // 2)
        return remote(xbuf.at[step, rows, :], part(step + 4, 2 - q, sub), relay_sem.at[q // 2, n], recv_sem.at[n, 2 - q],
                      ynbr if q == 0 else xnbr)

    def await_recv(step, q, sub=None):
        n = sem_of(step, sub)
        remote(part(step, q, sub), part(step, q, sub), fwd_sem.at[n, 0], recv_sem.at[n, q], partner).wait_recv()

    for i in range(4):
        xsend(i).start()
        ysend(i).start()
        if i == 0:
            pair_copy.start()

    def dot(a, b):
        return jnp.dot(a, b, preferred_element_type=F32)

    def dot_t(a, b):
        return lax.dot_general(a, b, (((0,), (0,)), ((), ())), preferred_element_type=F32)

    def project_q(step):
        q = dot(xbuf[step], wq[...])
        for h in range(nh):
            qt[h, :, step * tok:(step + 1) * tok] = q[:, h * HEAD:(h + 1) * HEAD].T.astype(BF16)

    def project_kv(step, sub=None):
        rows = slice(0, tok) if sub is None else slice(sub * tok // 2, (sub + 1) * tok // 2)
        keys = slice(0, rows.stop - rows.start)
        xs = xbuf[step, rows, :]
        kbuf[keys, :] = dot(xs, wk[...]).astype(BF16)
        vbuf[keys, :] = dot(xs, wv[...]).astype(BF16)

    def attend(keys=tok, qs=slice(0, 2 * tok), after=None):
        def logits(h):
            return dot(kbuf[0:keys, h * HEAD:(h + 1) * HEAD], qt[h, :, qs])

        s = logits(0)
        for h in range(nh):
            s_next = logits(h + 1) if h + 1 < nh else None
            m_old = mrow[h, :, qs]
            m_new = jnp.maximum(m_old, jnp.max(s, axis=0, keepdims=True))
            p = jnp.exp2((s - m_new) * scale)
            a = jnp.exp2((m_old - m_new) * scale)
            l_new = lrow[h, :, qs] * a + jnp.sum(p, axis=0, keepdims=True)
            o_new = acc[h, :, qs] * a + dot_t(vbuf[0:keys, h * HEAD:(h + 1) * HEAD], p.astype(BF16))
            if after is None:
                lrow[h, :, qs] = l_new
                mrow[h, :, qs] = m_new
                acc[h, :, qs] = o_new
            else:
                after(h, (o_new / l_new).astype(BF16))
            s = s_next

    acc[...] = jnp.zeros_like(acc)
    lrow[...] = jnp.zeros_like(lrow)
    mrow[...] = jnp.full(mrow.shape, -jnp.inf, F32)

    wq_copy.wait()
    project_q(0)
    wk_copy.wait()
    wv_copy.wait()
    wo_copy.start()
    project_kv(0)
    pair_copy.wait_recv()
    project_q(1)
    attend()
    project_kv(1)

    def body(step, carry):
        await_recv(step, 0)
        await_recv(step, 2)
        fwd(step, 0).start()
        fwd(step, 2).start()

        @pl.when(step == 2)
        def _():
            relay(2, 2).start()
            relay(0, 2).start()

        @pl.when(step == 3)
        def _():
            for sub in range(2):
                relay(2, 3, sub).start()
                relay(0, 3, sub).start()

        attend()
        await_recv(step, 1)
        await_recv(step, 3)
        project_kv(step)
        return carry

    lax.fori_loop(2, 7, body, 0)
    for sub in range(2):
        await_recv(7, 0, sub)
        await_recv(7, 2, sub)
        fwd(7, 0, sub).start()
        fwd(7, 2, sub).start()
        if sub == 0:
            attend()
        else:
            attend(keys=tok // 2)
        await_recv(7, 1, sub)
        await_recv(7, 3, sub)
        project_kv(7, sub)

    def osend_copy(h):
        return remote(osend.at[h], oother.at[h], osend_sem.at[h], orecv_sem.at[h], partner)

    def give(h, o):
        osend[h] = o
        if h > 0:
            osend_copy(h - 1).start()

    def keep(h, o):
        oown[h * HEAD:(h + 1) * HEAD, :] = o
        if h == 0:
            osend_copy(nh - 1).start()

    attend(keys=tok // 2, qs=slice(tok, 2 * tok), after=give)
    wo_copy.wait()
    attend(keys=tok // 2, qs=slice(0, tok), after=keep)
    own_rows_w = pl.ds(pl.multiple_of(core * half, HEAD), half)
    other_rows_w = pl.ds(pl.multiple_of((1 - core) * half, HEAD), half)
    yacc[...] = dot_t(oown[...], wo[own_rows_w, :])
    for h in range(nh):
        osend_copy(h).wait_recv()
    y_ref[...] = (yacc[...] + dot_t(oother[...].reshape(half, tok), wo[other_rows_w, :])).astype(BF16)

    pair_copy.wait_send()
    for i in range(4):
        xsend(i).wait_send()
        ysend(i).wait_send()
    for step, sub in [(s, None) for s in range(2, 7)] + [(7, 0), (7, 1)]:
        fwd(step, 0, sub).wait_send()
        fwd(step, 2, sub).wait_send()
    for step, sub in [(2, None), (3, 0), (3, 1)]:
        relay(0, step, sub).wait_send()
        relay(2, step, sub).wait_send()
    for h in range(nh):
        osend_copy(h).wait_send()


def solution(mesh):
    def block(x, w_qkv, w_o):
        tok, width = x.shape[1], x.shape[2]
        half = width // 2
        nh = half // HEAD
        any_spec = pl.BlockSpec(memory_space=pl.ANY)
        dma = pltpu.SemaphoreType.DMA
        y = pl.pallas_call(
            kernel,
            out_shape=jax.ShapeDtypeStruct((tok, width), BF16),
            in_specs=[any_spec] * 3,
            out_specs=pl.BlockSpec(memory_space=pltpu.VMEM),
            scratch_shapes=[
                pltpu.VMEM((8, tok, width), BF16),
                pltpu.VMEM((width, half), BF16),
                pltpu.VMEM((width, half), BF16),
                pltpu.VMEM((width, half), BF16),
                pltpu.VMEM((width, width), BF16),
                pltpu.VMEM((nh, HEAD, 2 * tok), BF16),
                pltpu.VMEM((tok, half), BF16),
                pltpu.VMEM((tok, half), BF16),
                pltpu.VMEM((nh, HEAD, 2 * tok), F32),
                pltpu.VMEM((nh, 1, 2 * tok), F32),
                pltpu.VMEM((nh, 1, 2 * tok), F32),
                pltpu.VMEM((nh, HEAD, tok), BF16),
                pltpu.VMEM((half, tok), BF16),
                pltpu.VMEM((nh, HEAD, tok), BF16),
                pltpu.VMEM((tok, width), F32),
                dma((4,)), dma(()), dma(()), dma((2, 4)), dma((9, 2)), dma((2, 9)), dma((nh,)),
                dma(()), dma((9, 4)), dma((nh,)),
            ],
            compiler_params=pltpu.CompilerParams(
                collective_id=0, has_side_effects=True, vmem_limit_bytes=53 * 1024 * 1024),
            name="gather_attend",
        )(x[0], w_qkv, w_o.reshape(width, width))
        return y[None]

    return jax.shard_map(
        block, mesh=mesh,
        in_specs=(P("dp", ("cx", "cy"), None), P(None, None), P(None, None, None)),
        out_specs=P("dp", ("cx", "cy"), None), check_vma=False)
```

```python
import functools
import math

import jax
import jax.numpy as jnp
from jax import lax
from jax.experimental import pallas as pl
from jax.experimental.pallas import tpu as pltpu
from jax.sharding import PartitionSpec as P

MESH = pl.DeviceIdType.MESH
BF16, F32 = jnp.bfloat16, jnp.float32
HEAD = 128


def kernel(x_hbm, wqkv_hbm, wo_hbm, y_ref,
           xbuf, wq, wk, wv, wo, qt, kbuf, vbuf, acc, mrow, lrow, osend, oown, oother, yacc,
           w_sem, own_sem, pair_sem, send_sem, fwd_sem, relay_sem, osend_sem,
           precv_sem, recv_sem, orecv_sem):
    tok, width = x_hbm.shape
    half = width // 2
    nh = half // HEAD
    quarter = tok // 4
    scale = math.log2(math.e) / math.sqrt(HEAD)

    dp, cx, cy = lax.axis_index("dp"), lax.axis_index("cx"), lax.axis_index("cy")
    core = lax.rem(cy, 2)
    partner = (dp, cx, cy + 1 - 2 * core)
    xnbr = (dp, cx, lax.rem(cy + 2, 4))
    ynbr = (dp, 1 - cx, cy)

    def wcopy(i, dst):
        cols = pl.ds(pl.multiple_of(i * width + core * half, HEAD), half)
        return pltpu.make_async_copy(wqkv_hbm.at[:, cols], dst, w_sem.at[i])

    xload = pltpu.make_async_copy(x_hbm, xbuf.at[0], own_sem)
    wq_copy, wk_copy, wv_copy = wcopy(0, wq), wcopy(1, wk), wcopy(2, wv)
    wo_copy = pltpu.make_async_copy(wo_hbm, wo, w_sem.at[3])
    xload.start()

    barrier = pltpu.get_barrier_semaphore()
    for nbr in (partner, xnbr, ynbr):
        pl.semaphore_signal(barrier, inc=1, device_id=nbr, device_id_type=MESH)
    xload.wait()
    wq_copy.start()
    wk_copy.start()
    wv_copy.start()
    pl.semaphore_wait(barrier, 3)

    def remote(src, dst, ssem, rsem, dev):
        return pltpu.make_async_remote_copy(src_ref=src, dst_ref=dst, send_sem=ssem, recv_sem=rsem,
                                            device_id=dev, device_id_type=MESH)

    def part(step, q, sub=None):
        if sub is None:
            return xbuf.at[step, pl.ds(q * quarter, quarter), :]
        return xbuf.at[step, pl.ds(sub * 2 * quarter + q * (quarter // 2), quarter // 2), :]

    def own_rows(i):
        start = i * quarter
        if not isinstance(i, int):
            start = pl.multiple_of(start, quarter)
        return xbuf.at[0, pl.ds(start, quarter), :]

    def xsend(i):
        return remote(own_rows((i + 2) % 4 if isinstance(i, int) else lax.rem(i + 2, 4)), part(2 + i, 0), send_sem.at[0, i], recv_sem.at[2 + i, 0], xnbr)

    def ysend(i):
        return remote(own_rows(i), part(2 + i, 2), send_sem.at[1, i], recv_sem.at[2 + i, 2], ynbr)

    pair_copy = remote(xbuf.at[0], xbuf.at[1], pair_sem, precv_sem, partner)

    def sem_of(step, sub):
        return step if not sub else step + sub

    def fwd(step, q, sub=None):
        n = sem_of(step, sub)
        return remote(part(step, q, sub), part(step, q + 1, sub), fwd_sem.at[n, q // 2], recv_sem.at[n, q + 1], partner)

    def relay(q, step, sub=None):
        n = sem_of(step + 4, sub)
        rows = pl.ds(q * quarter + (sub or 0) * (quarter // 2), quarter if sub is None else quarter // 2)
        return remote(xbuf.at[step, rows, :], part(step + 4, 2 - q, sub), relay_sem.at[q // 2, n], recv_sem.at[n, 2 - q],
                      ynbr if q == 0 else xnbr)

    def await_recv(step, q, sub=None):
        n = sem_of(step, sub)
        remote(part(step, q, sub), part(step, q, sub), fwd_sem.at[n, 0], recv_sem.at[n, q], partner).wait_recv()

    for i in range(2):
        xsend(i).start()
        ysend(i).start()
        if i == 0:
            pair_copy.start()

    def dot(a, b):
        return jnp.dot(a, b, preferred_element_type=F32)

    def dot_t(a, b):
        return lax.dot_general(a, b, (((0,), (0,)), ((), ())), preferred_element_type=F32)

    def project_q(step):
        q = dot(xbuf[step], wq[...])
        for h in range(nh):
            qt[h, :, step * tok:(step + 1) * tok] = q[:, h * HEAD:(h + 1) * HEAD].T.astype(BF16)

    def project_kv(step, sub=None):
        rows = slice(0, tok) if sub is None else slice(sub * tok // 2, (sub + 1) * tok // 2)
        keys = slice(0, rows.stop - rows.start)
        xs = xbuf[step, rows, :]
        kbuf[keys, :] = dot(xs, wk[...]).astype(BF16)
        vbuf[keys, :] = dot(xs, wv[...]).astype(BF16)

    def attend(keys=tok, qs=slice(0, 2 * tok), after=None):
        def logits(h):
            return dot(kbuf[0:keys, h * HEAD:(h + 1) * HEAD], qt[h, :, qs])

        s = logits(0)
        for h in range(nh):
            s_next = logits(h + 1) if h + 1 < nh else None
            m_old = mrow[h, :, qs]
            m_new = jnp.maximum(m_old, jnp.max(s, axis=0, keepdims=True))
            p = jnp.exp2((s - m_new) * scale)
            a = jnp.exp2((m_old - m_new) * scale)
            l_new = lrow[h, :, qs] * a + jnp.sum(p, axis=0, keepdims=True)
            o_new = acc[h, :, qs] * a + dot_t(vbuf[0:keys, h * HEAD:(h + 1) * HEAD], p.astype(BF16))
            if after is None:
                lrow[h, :, qs] = l_new
                mrow[h, :, qs] = m_new
                acc[h, :, qs] = o_new
            else:
                after(h, (o_new / l_new).astype(BF16))
            s = s_next

    acc[...] = jnp.zeros_like(acc)
    lrow[...] = jnp.zeros_like(lrow)
    mrow[...] = jnp.full(mrow.shape, -jnp.inf, F32)

    wq_copy.wait()
    project_q(0)
    wk_copy.wait()
    wv_copy.wait()
    wo_copy.start()
    project_kv(0)
    pair_copy.wait_recv()
    project_q(1)
    attend()
    project_kv(1)

    def body(step, carry):
        await_recv(step, 0)
        await_recv(step, 2)
        fwd(step, 0).start()
        fwd(step, 2).start()

        @pl.when(step < 4)
        def _():
            xsend(step).start()
            ysend(step).start()

        @pl.when(step == 4)
        def _():
            relay(2, 2).start()
            relay(0, 2).start()

        @pl.when(step == 5)
        def _():
            relay(2, 3, 0).start()
            relay(0, 3, 0).start()

        @pl.when(step == 6)
        def _():
            relay(2, 3, 1).start()
            relay(0, 3, 1).start()

        attend()
        await_recv(step, 1)
        await_recv(step, 3)
        project_kv(step)
        return carry

    lax.fori_loop(2, 7, body, 0)
    for sub in range(2):
        await_recv(7, 0, sub)
        await_recv(7, 2, sub)
        fwd(7, 0, sub).start()
        fwd(7, 2, sub).start()
        if sub == 0:
            attend()
        else:
            attend(keys=tok // 2)
        await_recv(7, 1, sub)
        await_recv(7, 3, sub)
        project_kv(7, sub)

    def osend_copy(h):
        return remote(osend.at[h], oother.at[h], osend_sem.at[h], orecv_sem.at[h], partner)

    def give(h, o):
        osend[h] = o
        if h > 0:
            osend_copy(h - 1).start()

    def keep(h, o):
        oown[h * HEAD:(h + 1) * HEAD, :] = o
        if h == 0:
            osend_copy(nh - 1).start()

    attend(keys=tok // 2, qs=slice(tok, 2 * tok), after=give)
    wo_copy.wait()
    attend(keys=tok // 2, qs=slice(0, tok), after=keep)
    own_rows_w = pl.ds(pl.multiple_of(core * half, HEAD), half)
    other_rows_w = pl.ds(pl.multiple_of((1 - core) * half, HEAD), half)
    yacc[...] = dot_t(oown[...], wo[own_rows_w, :])
    for h in range(nh):
        osend_copy(h).wait_recv()
    y_ref[...] = (yacc[...] + dot_t(oother[...].reshape(half, tok), wo[other_rows_w, :])).astype(BF16)

    pair_copy.wait_send()
    for i in range(4):
        xsend(i).wait_send()
        ysend(i).wait_send()
    for step, sub in [(s, None) for s in range(2, 7)] + [(7, 0), (7, 1)]:
        fwd(step, 0, sub).wait_send()
        fwd(step, 2, sub).wait_send()
    for step, sub in [(2, None), (3, 0), (3, 1)]:
        relay(0, step, sub).wait_send()
        relay(2, step, sub).wait_send()
    for h in range(nh):
        osend_copy(h).wait_send()


def solution(mesh):
    def block(x, w_qkv, w_o):
        tok, width = x.shape[1], x.shape[2]
        half = width // 2
        nh = half // HEAD
        any_spec = pl.BlockSpec(memory_space=pl.ANY)
        dma = pltpu.SemaphoreType.DMA
        y = pl.pallas_call(
            kernel,
            out_shape=jax.ShapeDtypeStruct((tok, width), BF16),
            in_specs=[any_spec] * 3,
            out_specs=pl.BlockSpec(memory_space=pltpu.VMEM),
            scratch_shapes=[
                pltpu.VMEM((8, tok, width), BF16),
                pltpu.VMEM((width, half), BF16),
                pltpu.VMEM((width, half), BF16),
                pltpu.VMEM((width, half), BF16),
                pltpu.VMEM((width, width), BF16),
                pltpu.VMEM((nh, HEAD, 2 * tok), BF16),
                pltpu.VMEM((tok, half), BF16),
                pltpu.VMEM((tok, half), BF16),
                pltpu.VMEM((nh, HEAD, 2 * tok), F32),
                pltpu.VMEM((nh, 1, 2 * tok), F32),
                pltpu.VMEM((nh, 1, 2 * tok), F32),
                pltpu.VMEM((nh, HEAD, tok), BF16),
                pltpu.VMEM((half, tok), BF16),
                pltpu.VMEM((nh, HEAD, tok), BF16),
                pltpu.VMEM((tok, width), F32),
                dma((4,)), dma(()), dma(()), dma((2, 4)), dma((9, 2)), dma((2, 9)), dma((nh,)),
                dma(()), dma((9, 4)), dma((nh,)),
            ],
            compiler_params=pltpu.CompilerParams(
                collective_id=0, has_side_effects=True, vmem_limit_bytes=53 * 1024 * 1024),
            name="gather_attend",
        )(x[0], w_qkv, w_o.reshape(width, width))
        return y[None]

    return jax.shard_map(
        block, mesh=mesh,
        in_specs=(P("dp", ("cx", "cy"), None), P(None, None), P(None, None, None)),
        out_specs=P("dp", ("cx", "cy"), None), check_vma=False)
```

```python
import functools
import math

import jax
import jax.numpy as jnp
from jax import lax
from jax.experimental import pallas as pl
from jax.experimental.pallas import tpu as pltpu
from jax.sharding import PartitionSpec as P

MESH = pl.DeviceIdType.MESH
BF16, F32 = jnp.bfloat16, jnp.float32
HEAD = 128


def kernel(x_hbm, wqkv_hbm, wo_hbm, y_ref,
           xbuf, wq, wk, wv, wo, qt, kbuf0, kbuf1, vbuf0, vbuf1, acc, mrow, lrow, osend, oown, oother, yacc,
           w_sem, own_sem, pair_sem, send_sem, fwd_sem, relay_sem, osend_sem,
           precv_sem, recv_sem, orecv_sem):
    tok, width = x_hbm.shape
    half = width // 2
    nh = half // HEAD
    quarter = tok // 4
    scale = math.log2(math.e) / math.sqrt(HEAD)

    dp, cx, cy = lax.axis_index("dp"), lax.axis_index("cx"), lax.axis_index("cy")
    core = lax.rem(cy, 2)
    partner = (dp, cx, cy + 1 - 2 * core)
    xnbr = (dp, cx, lax.rem(cy + 2, 4))
    ynbr = (dp, 1 - cx, cy)

    def wcopy(i, dst):
        cols = pl.ds(pl.multiple_of(i * width + core * half, HEAD), half)
        return pltpu.make_async_copy(wqkv_hbm.at[:, cols], dst, w_sem.at[i])

    xload = pltpu.make_async_copy(x_hbm, xbuf.at[0], own_sem)
    wq_copy, wk_copy, wv_copy = wcopy(0, wq), wcopy(1, wk), wcopy(2, wv)
    wo_copy = pltpu.make_async_copy(wo_hbm, wo, w_sem.at[3])
    xload.start()

    barrier = pltpu.get_barrier_semaphore()
    for nbr in (partner, xnbr, ynbr):
        pl.semaphore_signal(barrier, inc=1, device_id=nbr, device_id_type=MESH)
    xload.wait()
    wq_copy.start()
    wk_copy.start()
    wv_copy.start()
    pl.semaphore_wait(barrier, 3)

    def remote(src, dst, ssem, rsem, dev):
        return pltpu.make_async_remote_copy(src_ref=src, dst_ref=dst, send_sem=ssem, recv_sem=rsem,
                                            device_id=dev, device_id_type=MESH)

    def part(step, q, sub=None):
        if sub is None:
            return xbuf.at[step, pl.ds(q * quarter, quarter), :]
        return xbuf.at[step, pl.ds(sub * 2 * quarter + q * (quarter // 2), quarter // 2), :]

    def own_rows(i):
        start = i * quarter
        if not isinstance(i, int):
            start = pl.multiple_of(start, quarter)
        return xbuf.at[0, pl.ds(start, quarter), :]

    def xsend(i):
        return remote(own_rows((i + 2) % 4 if isinstance(i, int) else lax.rem(i + 2, 4)), part(2 + i, 0), send_sem.at[0, i], recv_sem.at[2 + i, 0], xnbr)

    def ysend(i):
        return remote(own_rows(i), part(2 + i, 2), send_sem.at[1, i], recv_sem.at[2 + i, 2], ynbr)

    pair_copy = remote(xbuf.at[0], xbuf.at[1], pair_sem, precv_sem, partner)

    def sem_of(step, sub):
        return step if not sub else step + sub

    def fwd(step, q, sub=None):
        n = sem_of(step, sub)
        return remote(part(step, q, sub), part(step, q + 1, sub), fwd_sem.at[n, q // 2], recv_sem.at[n, q + 1], partner)

    def relay(q, step, sub=None):
        n = sem_of(step + 4, sub)
        rows = pl.ds(q * quarter + (sub or 0) * (quarter // 2), quarter if sub is None else quarter // 2)
        return remote(xbuf.at[step, rows, :], part(step + 4, 2 - q, sub), relay_sem.at[q // 2, n], recv_sem.at[n, 2 - q],
                      ynbr if q == 0 else xnbr)

    def await_recv(step, q, sub=None):
        n = sem_of(step, sub)
        remote(part(step, q, sub), part(step, q, sub), fwd_sem.at[n, 0], recv_sem.at[n, q], partner).wait_recv()

    out_x = [xsend(i) for i in range(4)] + [relay(2, 2), relay(2, 3, 0), relay(2, 3, 1)]
    out_y = [ysend(i) for i in range(4)] + [relay(0, 2), relay(0, 3, 0), relay(0, 3, 1)]
    depth = 3
    for i in range(depth):
        out_x[i].start()
        out_y[i].start()
        if i == 0:
            pair_copy.start()

    chunks = [(0, None), (1, None)] + [(s, None) for s in range(2, 7)] + [(7, 0), (7, 1)]
    kbufs, vbufs = (kbuf0, kbuf1), (vbuf0, vbuf1)

    def nkeys(c):
        return tok if chunks[c][1] is None else tok // 2

    def arrive(c):
        step, sub = chunks[c]
        await_recv(step, 0, sub)
        await_recv(step, 2, sub)
        fwd(step, 0, sub).start()
        fwd(step, 2, sub).start()
        i = c - 2 + depth
        if i < len(out_x):
            out_x[i].start()
            out_y[i].start()

    def twins(c):
        step, sub = chunks[c]
        await_recv(step, 1, sub)
        await_recv(step, 3, sub)

    def dot(a, b):
        return jnp.dot(a, b, preferred_element_type=F32)

    def dot_t(a, b):
        return lax.dot_general(a, b, (((0,), (0,)), ((), ())), preferred_element_type=F32)

    def project_q(step):
        q = dot(xbuf[step], wq[...])
        for h in range(nh):
            qt[h, :, step * tok:(step + 1) * tok] = q[:, h * HEAD:(h + 1) * HEAD].T.astype(BF16)

    piece = 2 * HEAD

    def project_pieces(c):
        step, sub = chunks[c]
        n = nkeys(c)
        row0 = 0 if not sub else sub * n
        for w, buf in ((wk, kbufs[c % 2]), (wv, vbufs[c % 2])):
            for j in range(half // piece):
                cols = slice(j * piece, (j + 1) * piece)
                buf[0:n, cols] = dot(xbuf[step, row0:row0 + n, :], w[:, cols]).astype(BF16)
                yield

    def attend_heads(c, qs=slice(0, 2 * tok), after=None):
        n = nkeys(c)
        kb, vb = kbufs[c % 2], vbufs[c % 2]

        def logits(h):
            return dot(kb[0:n, h * HEAD:(h + 1) * HEAD], qt[h, :, qs])

        s = logits(0)
        for h in range(nh):
            s_next = logits(h + 1) if h + 1 < nh else None
            m_old = mrow[h, :, qs]
            m_new = jnp.maximum(m_old, jnp.max(s, axis=0, keepdims=True))
            p = jnp.exp2((s - m_new) * scale)
            a = jnp.exp2((m_old - m_new) * scale)
            l_new = lrow[h, :, qs] * a + jnp.sum(p, axis=0, keepdims=True)
            o_new = acc[h, :, qs] * a + dot_t(vb[0:n, h * HEAD:(h + 1) * HEAD], p.astype(BF16))
            if after is None:
                lrow[h, :, qs] = l_new
                mrow[h, :, qs] = m_new
                acc[h, :, qs] = o_new
            else:
                after(h, (o_new * (1.0 / l_new)).astype(BF16))
            s = s_next
            yield

    def run(*gens):
        gens = list(gens)
        while gens:
            for g in list(gens):
                if next(g, gens) is gens:
                    gens.remove(g)

    acc[...] = jnp.zeros_like(acc)
    lrow[...] = jnp.zeros_like(lrow)
    mrow[...] = jnp.full(mrow.shape, -jnp.inf, F32)

    wq_copy.wait()
    project_q(0)
    wk_copy.wait()
    wv_copy.wait()
    wo_copy.start()
    run(project_pieces(0))
    pair_copy.wait_recv()
    project_q(1)
    run(project_pieces(1), attend_heads(0))
    for c in range(2, 6):
        arrive(c)
        twins(c)
        run(project_pieces(c), attend_heads(c - 1))
    arrive(6)
    run(attend_heads(5))
    twins(6)
    pair_copy.wait_send()
    for i in range(4):
        xsend(i).wait_send()
        ysend(i).wait_send()
    for c in range(2, 6):
        fwd(*[chunks[c][0], 0]).wait_send()
        fwd(*[chunks[c][0], 2]).wait_send()
    arrive(7)
    run(project_pieces(6))
    twins(7)
    for step in (2, 3):
        sub = None if step == 2 else 0
        relay(0, step, sub).wait_send()
        relay(2, step, sub).wait_send()
    fwd(6, 0).wait_send()
    fwd(6, 2).wait_send()
    arrive(8)
    run(project_pieces(7), attend_heads(6))
    twins(8)
    for q in (0, 2):
        relay(q, 3, 1).wait_send()
        fwd(7, q, 0).wait_send()
        fwd(7, q, 1).wait_send()
    run(project_pieces(8), attend_heads(7))

    def osend_copy(h):
        return remote(osend.at[h], oother.at[h], osend_sem.at[h], orecv_sem.at[h], partner)

    def give(h, o):
        osend[h] = o
        if h > 0:
            osend_copy(h - 1).start()

    def keep(h, o):
        oown[h * HEAD:(h + 1) * HEAD, :] = o
        if h == 0:
            osend_copy(nh - 1).start()

    wo_copy.wait()
    run(attend_heads(8, slice(tok, 2 * tok), give))
    run(attend_heads(8, slice(0, tok), keep))
    own_rows_w = pl.ds(pl.multiple_of(core * half, HEAD), half)
    other_rows_w = pl.ds(pl.multiple_of((1 - core) * half, HEAD), half)
    yacc[...] = dot_t(oown[...], wo[own_rows_w, :])
    for h in range(nh):
        osend_copy(h).wait_recv()
    y_ref[...] = (yacc[...] + dot_t(oother[...].reshape(half, tok), wo[other_rows_w, :])).astype(BF16)

    for h in range(nh):
        osend_copy(h).wait_send()


def solution(mesh):
    def block(x, w_qkv, w_o):
        tok, width = x.shape[1], x.shape[2]
        half = width // 2
        nh = half // HEAD
        any_spec = pl.BlockSpec(memory_space=pl.ANY)
        dma = pltpu.SemaphoreType.DMA
        y = pl.pallas_call(
            kernel,
            out_shape=jax.ShapeDtypeStruct((tok, width), BF16),
            in_specs=[any_spec] * 3,
            out_specs=pl.BlockSpec(memory_space=pltpu.VMEM),
            scratch_shapes=[
                pltpu.VMEM((8, tok, width), BF16),
                pltpu.VMEM((width, half), BF16),
                pltpu.VMEM((width, half), BF16),
                pltpu.VMEM((width, half), BF16),
                pltpu.VMEM((width, width), BF16),
                pltpu.VMEM((nh, HEAD, 2 * tok), BF16),
                pltpu.VMEM((tok, half), BF16),
                pltpu.VMEM((tok, half), BF16),
                pltpu.VMEM((tok, half), BF16),
                pltpu.VMEM((tok, half), BF16),
                pltpu.VMEM((nh, HEAD, 2 * tok), F32),
                pltpu.VMEM((nh, 1, 2 * tok), F32),
                pltpu.VMEM((nh, 1, 2 * tok), F32),
                pltpu.VMEM((nh, HEAD, tok), BF16),
                pltpu.VMEM((half, tok), BF16),
                pltpu.VMEM((nh, HEAD, tok), BF16),
                pltpu.VMEM((tok, width), F32),
                dma((4,)), dma(()), dma(()), dma((2, 4)), dma((9, 2)), dma((2, 9)), dma((nh,)),
                dma(()), dma((9, 4)), dma((nh,)),
            ],
            compiler_params=pltpu.CompilerParams(
                collective_id=0, has_side_effects=True, vmem_limit_bytes=53 * 1024 * 1024),
            name="gather_attend",
        )(x[0], w_qkv, w_o.reshape(width, width))
        return y[None]

    return jax.shard_map(
        block, mesh=mesh,
        in_specs=(P("dp", ("cx", "cy"), None), P(None, None), P(None, None, None)),
        out_specs=P("dp", ("cx", "cy"), None), check_vma=False)
```

```python
import math

import jax
import jax.numpy as jnp
from jax import lax
from jax.experimental import pallas as pl
from jax.experimental.pallas import tpu as pltpu
from jax.sharding import PartitionSpec as P

MESH = pl.DeviceIdType.MESH
BF16, F32 = jnp.bfloat16, jnp.float32
HEAD = 128


def kernel(x_hbm, wqkv_hbm, wo_hbm, y_ref,
           xbuf, wq, wk, wv, wo, qt, kbuf0, kbuf1, vbuf0, vbuf1, acc, mrow, lrow, osend, oown, oother, facc,
           w_sem, x_sem, pair_sem, send_sem, osend_sem, link_sem, twin_sem, orecv_sem):
    tok, width = x_hbm.shape
    half = width // 2
    nh = half // HEAD
    quarter = tok // 4
    scale = math.log2(math.e) / math.sqrt(HEAD)

    dp, cx, cy = lax.axis_index("dp"), lax.axis_index("cx"), lax.axis_index("cy")
    core = lax.rem(cy, 2)
    partner = (dp, cx, cy + 1 - 2 * core)
    xnbr = (dp, cx, lax.rem(cy + 2, 4))
    ynbr = (dp, 1 - cx, cy)

    def wcopy(i, dst):
        cols = pl.ds(pl.multiple_of(i * width + core * half, HEAD), half)
        return pltpu.make_async_copy(wqkv_hbm.at[:, cols], dst, w_sem.at[i])

    wq_copy, wk_copy, wv_copy = wcopy(0, wq), wcopy(1, wk), wcopy(2, wv)
    wo_copy = pltpu.make_async_copy(wo_hbm, wo, w_sem.at[3])

    def own_rows(i, n=1):
        return xbuf.at[0, pl.ds(i * quarter, n * quarter), :]

    for i in (2, 0, 3, 1):
        pltpu.make_async_copy(x_hbm.at[pl.ds(i * quarter, quarter), :], own_rows(i), x_sem.at[i % 2]).start()

    def xload_wait(i):
        pltpu.make_async_copy(x_hbm.at[pl.ds(0, 2 * quarter), :], own_rows(0, 2), x_sem.at[i]).wait()

    barrier = pltpu.get_barrier_semaphore()
    for nbr in (partner, xnbr, ynbr):
        pl.semaphore_signal(barrier, inc=1, device_id=nbr, device_id_type=MESH)
    acc[...] = jnp.zeros_like(acc)
    lrow[...] = jnp.zeros_like(lrow)
    mrow[...] = jnp.full(mrow.shape, -jnp.inf, F32)
    wq_copy.start()
    xload_wait(0)
    pl.semaphore_wait(barrier, 3)

    pieces = [(c, slice(0, width)) for c in range(2, 7)] + [(7, slice(0, half)), (7, slice(half, width))]

    def part(c, q, cols):
        return xbuf.at[c, q * quarter:(q + 1) * quarter, cols]

    def remote(src, dst, ssem, rsem, dev):
        return pltpu.make_async_remote_copy(src_ref=src, dst_ref=dst, send_sem=ssem, recv_sem=rsem,
                                            device_id=dev, device_id_type=MESH)

    def link_copy(i, q):
        c, cols = pieces[i]
        dev = xnbr if q == 0 else ynbr
        if c < 6:
            src = own_rows((c if q == 0 else c - 2) % 4)
        else:
            src = part(c - 4, 2 - q, cols)
        return remote(src, part(c, q, cols), send_sem, link_sem.at[i], dev)

    def twin_copy(i, q):
        c, cols = pieces[i]
        return remote(part(c, q, cols), part(c, q + 1, cols), send_sem, twin_sem.at[i], partner)

    pair_copy = remote(xbuf.at[0], xbuf.at[1], send_sem, pair_sem, partner)
    depth = 3

    def send(i):
        if i < len(pieces):
            link_copy(i, 0).start()
            link_copy(i, 2).start()

    def both_parts(i, sems):
        c, cols = pieces[i]
        both = xbuf.at[c, 0:2 * quarter, cols]
        return remote(both, both, send_sem, sems.at[i], partner)

    def arrive(i):
        both_parts(i, link_sem).wait_recv()
        twin_copy(i, 0).start()
        twin_copy(i, 2).start()
        send(i + depth)

    def twins(i):
        both_parts(i, twin_sem).wait_recv()

    send(0)
    xload_wait(1)
    for i in range(1, depth):
        send(i)
    pair_copy.start()
    wk_copy.start()
    wv_copy.start()

    def dot(a, b):
        return jnp.dot(a, b, preferred_element_type=F32)

    def dot_t(a, b):
        return lax.dot_general(a, b, (((0,), (0,)), ((), ())), preferred_element_type=F32)

    kbufs, vbufs = (kbuf0, kbuf1), (vbuf0, vbuf1)

    def project_q(c):
        q = dot(xbuf[c], wq[...])
        for h in range(nh):
            qt[h, :, c * tok:(c + 1) * tok] = q[:, h * HEAD:(h + 1) * HEAD].T.astype(BF16)

    def project(c):
        xs = xbuf[c]
        kbufs[c % 2][...] = dot(xs, wk[...]).astype(BF16)
        vbufs[c % 2][...] = dot(xs, wv[...]).astype(BF16)

    def project_first(c):
        xs = xbuf[c, :, 0:half]
        facc[:, 0:half] = dot(xs, wk[0:half, :])
        facc[:, half:] = dot(xs, wv[0:half, :])

    def project_second(c):
        xs = xbuf[c, :, half:]
        kbufs[c % 2][...] = (facc[:, 0:half] + dot(xs, wk[half:, :])).astype(BF16)
        vbufs[c % 2][...] = (facc[:, half:] + dot(xs, wv[half:, :])).astype(BF16)

    def attend(c, heads=range(nh), qs=slice(0, 2 * tok), out=None):
        kb, vb = kbufs[c % 2], vbufs[c % 2]

        def logits(h):
            return dot(kb[:, h * HEAD:(h + 1) * HEAD], qt[h, :, qs])

        s = logits(heads[0])
        for h in heads:
            s_next = logits(h + 1) if h + 1 in heads else None
            m_old = mrow[h, :, qs]
            m_new = jnp.maximum(m_old, jnp.max(s, axis=0, keepdims=True))
            p = jnp.exp2((s - m_new) * scale)
            a = jnp.exp2((m_old - m_new) * scale)
            l_new = lrow[h, :, qs] * a + jnp.sum(p, axis=0, keepdims=True)
            o_new = acc[h, :, qs] * a + dot_t(vb[:, h * HEAD:(h + 1) * HEAD], p.astype(BF16))
            if out is None:
                lrow[h, :, qs] = l_new
                mrow[h, :, qs] = m_new
                acc[h, :, qs] = o_new
            else:
                out[h * HEAD:(h + 1) * HEAD, :] = (o_new * (1.0 / l_new)).astype(BF16)
            s = s_next

    wq_copy.wait()
    project_q(0)
    wk_copy.wait()
    wv_copy.wait()
    wo_copy.start()
    project(0)
    pair_copy.wait_recv()
    project_q(1)
    project(1)
    arrive(0)
    attend(0)
    twins(0)
    project(2)
    arrive(1)
    attend(1)
    twins(1)
    project(3)
    attend(2)
    arrive(2)
    twins(2)
    project(4)
    attend(3)
    arrive(3)
    attend(4, range(0, 3))
    twins(3)
    project(5)
    attend(4, range(3, 6))
    attend(5, range(0, 3))
    arrive(4)
    attend(5, range(3, 6))
    twins(4)
    project(6)
    arrive(5)
    attend(6)
    arrive(6)
    twins(5)
    project_first(7)
    twins(6)
    project_second(7)
    attend(7, qs=slice(tok, 2 * tok), out=osend)
    wo_copy.wait()
    ocopy = remote(osend, oother, osend_sem, orecv_sem, partner)
    ocopy.start()
    attend(7, qs=slice(0, tok), out=oown)
    own_rows_w = pl.ds(pl.multiple_of(core * half, HEAD), half)
    other_rows_w = pl.ds(pl.multiple_of((1 - core) * half, HEAD), half)
    facc[...] = dot_t(oown[...], wo[own_rows_w, :])
    ocopy.wait_recv()
    y_ref[...] = (facc[...] + dot_t(oother[...], wo[other_rows_w, :])).astype(BF16)

    sent = xbuf.at[0:7]
    remote(sent, sent, send_sem, pair_sem, partner).wait_send()
    ocopy.wait_send()


def solution(mesh):
    def block(x, w_qkv, w_o):
        tok, width = x.shape[1], x.shape[2]
        half = width // 2
        nh = half // HEAD
        any_spec = pl.BlockSpec(memory_space=pl.ANY)
        dma = pltpu.SemaphoreType.DMA
        y = pl.pallas_call(
            kernel,
            out_shape=jax.ShapeDtypeStruct((tok, width), BF16),
            in_specs=[any_spec] * 3,
            out_specs=pl.BlockSpec(memory_space=pltpu.VMEM),
            scratch_shapes=[
                pltpu.VMEM((8, tok, width), BF16),
                pltpu.VMEM((width, half), BF16),
                pltpu.VMEM((width, half), BF16),
                pltpu.VMEM((width, half), BF16),
                pltpu.VMEM((width, width), BF16),
                pltpu.VMEM((nh, HEAD, 2 * tok), BF16),
                pltpu.VMEM((tok, half), BF16),
                pltpu.VMEM((tok, half), BF16),
                pltpu.VMEM((tok, half), BF16),
                pltpu.VMEM((tok, half), BF16),
                pltpu.VMEM((nh, HEAD, 2 * tok), F32),
                pltpu.VMEM((nh, 1, 2 * tok), F32),
                pltpu.VMEM((nh, 1, 2 * tok), F32),
                pltpu.VMEM((half, tok), BF16),
                pltpu.VMEM((half, tok), BF16),
                pltpu.VMEM((half, tok), BF16),
                pltpu.VMEM((tok, width), F32),
                dma((4,)), dma((2,)), dma(()), dma(()), dma(()), dma((7,)), dma((7,)), dma(()),
            ],
            compiler_params=pltpu.CompilerParams(
                collective_id=0, has_side_effects=True, vmem_limit_bytes=53 * 1024 * 1024),
            name="gather_attend",
        )(x[0], w_qkv, w_o.reshape(width, width))
        return y[None]

    return jax.shard_map(
        block, mesh=mesh,
        in_specs=(P("dp", ("cx", "cy"), None), P(None, None), P(None, None, None)),
        out_specs=P("dp", ("cx", "cy"), None), check_vma=False)
```

```python
import math

import jax
import jax.numpy as jnp
from jax import lax
from jax.experimental import pallas as pl
from jax.experimental.pallas import tpu as pltpu
from jax.sharding import PartitionSpec as P

MESH = pl.DeviceIdType.MESH
BF16, F32 = jnp.bfloat16, jnp.float32
HEAD = 128


def kernel(x_hbm, wqkv_hbm, wo_hbm, y_ref,
           xbuf, wq, wk, wv, wo, qt, kbuf0, kbuf1, vbuf0, vbuf1, acc, mrow, lrow, osend, oown, oother, facc,
           w_sem, x_sem, pair_sem, send_sem, osend_sem, link_sem, twin_sem, orecv_sem):
    tok, width = x_hbm.shape
    half = width // 2
    nh = half // HEAD
    quarter = tok // 4
    cut = 9 * HEAD
    scale = math.log2(math.e) / math.sqrt(HEAD)

    dp, cx, cy = lax.axis_index("dp"), lax.axis_index("cx"), lax.axis_index("cy")
    core = lax.rem(cy, 2)
    partner = (dp, cx, cy + 1 - 2 * core)
    xnbr = (dp, cx, lax.rem(cy + 2, 4))
    ynbr = (dp, 1 - cx, cy)

    def wcopy(i, dst):
        cols = pl.ds(pl.multiple_of(i * width + core * half, HEAD), half)
        return pltpu.make_async_copy(wqkv_hbm.at[:, cols], dst, w_sem.at[i])

    wq_copy, wk_copy, wv_copy = wcopy(0, wq), wcopy(1, wk), wcopy(2, wv)
    wo_copy = pltpu.make_async_copy(wo_hbm, wo, w_sem.at[3])

    def own_rows(i, n=1):
        return xbuf.at[0, pl.ds(i * quarter, n * quarter), :]

    for i in (2, 0, 3, 1):
        pltpu.make_async_copy(x_hbm.at[pl.ds(i * quarter, quarter), :], own_rows(i), x_sem.at[i % 2]).start()

    def xload_wait(i):
        pltpu.make_async_copy(x_hbm.at[pl.ds(0, 2 * quarter), :], own_rows(0, 2), x_sem.at[i]).wait()

    barrier = pltpu.get_barrier_semaphore()
    for nbr in (partner, xnbr, ynbr):
        pl.semaphore_signal(barrier, inc=1, device_id=nbr, device_id_type=MESH)
    acc[...] = jnp.zeros_like(acc)
    lrow[...] = jnp.zeros_like(lrow)
    mrow[...] = jnp.full(mrow.shape, -jnp.inf, F32)
    wq_copy.start()
    xload_wait(0)
    pl.semaphore_wait(barrier, 3)

    pieces = [(c, slice(0, width)) for c in range(2, 7)] + [(7, slice(0, cut)), (7, slice(cut, width))]

    def part(c, q, cols):
        return xbuf.at[c, q * quarter:(q + 1) * quarter, cols]

    def remote(src, dst, ssem, rsem, dev):
        return pltpu.make_async_remote_copy(src_ref=src, dst_ref=dst, send_sem=ssem, recv_sem=rsem,
                                            device_id=dev, device_id_type=MESH)

    def link_copy(i, q):
        c, cols = pieces[i]
        dev = xnbr if q == 0 else ynbr
        if c < 6:
            src = own_rows((c if q == 0 else c - 2) % 4)
        else:
            src = part(c - 4, 2 - q, cols)
        return remote(src, part(c, q, cols), send_sem, link_sem.at[i], dev)

    def twin_copy(i, q):
        c, cols = pieces[i]
        return remote(part(c, q, cols), part(c, q + 1, cols), send_sem, twin_sem.at[i], partner)

    pair_copy = remote(xbuf.at[0], xbuf.at[1], send_sem, pair_sem, partner)
    depth = 3

    def send(i):
        if i < len(pieces):
            link_copy(i, 0).start()
            link_copy(i, 2).start()

    def both_parts(i, sems):
        c, cols = pieces[i]
        both = xbuf.at[c, 0:2 * quarter, cols]
        return remote(both, both, send_sem, sems.at[i], partner)

    def arrive(i):
        both_parts(i, link_sem).wait_recv()
        twin_copy(i, 0).start()
        twin_copy(i, 2).start()
        if i == 1:
            send(i + 2)
        send(i + depth - (i < 1))

    def twins(i):
        both_parts(i, twin_sem).wait_recv()

    send(0)
    xload_wait(1)
    send(1)
    pair_copy.start()
    wk_copy.start()
    wv_copy.start()

    def dot(a, b):
        return jnp.dot(a, b, preferred_element_type=F32)

    def dot_t(a, b):
        return lax.dot_general(a, b, (((0,), (0,)), ((), ())), preferred_element_type=F32)

    kbufs, vbufs = (kbuf0, kbuf1), (vbuf0, vbuf1)

    def project_q(c):
        q = dot(xbuf[c], wq[...]).astype(BF16)
        for h in range(nh):
            qt[h, :, c * tok:(c + 1) * tok] = q[:, h * HEAD:(h + 1) * HEAD].T

    def project(c):
        xs = xbuf[c]
        kbufs[c % 2][...] = dot(xs, wk[...]).astype(BF16)
        vbufs[c % 2][...] = dot(xs, wv[...]).astype(BF16)

    def project_first(c):
        xs = xbuf[c, :, 0:cut]
        facc[:, 0:half] = dot(xs, wk[0:cut, :])
        facc[:, half:] = dot(xs, wv[0:cut, :])

    def project_second(c):
        xs = xbuf[c, :, cut:]
        kbufs[c % 2][...] = (facc[:, 0:half] + dot(xs, wk[cut:, :])).astype(BF16)
        vbufs[c % 2][...] = (facc[:, half:] + dot(xs, wv[cut:, :])).astype(BF16)

    def attend(c, heads=range(nh), last=False):
        kb, vb = kbufs[c % 2], vbufs[c % 2]

        def logits(h):
            return dot(kb[:, h * HEAD:(h + 1) * HEAD], qt[h])

        s = logits(heads[0])
        for h in heads:
            s_next = logits(h + 1) if h + 1 in heads else None
            m_old = mrow[h]
            m_new = jnp.maximum(m_old, jnp.max(s, axis=0, keepdims=True))
            p = jnp.exp2((s - m_new) * scale)
            a = jnp.exp2((m_old - m_new) * scale)
            l_new = lrow[h] * a + jnp.sum(p, axis=0, keepdims=True)
            o_new = acc[h] * a + dot_t(vb[:, h * HEAD:(h + 1) * HEAD], p.astype(BF16))
            if not last:
                lrow[h] = l_new
                mrow[h] = m_new
                acc[h] = o_new
            else:
                o = (o_new * (1.0 / l_new)).astype(BF16)
                oown[h * HEAD:(h + 1) * HEAD, :] = o[:, 0:tok]
                osend[h * HEAD:(h + 1) * HEAD, :] = o[:, tok:]
            s = s_next

    wq_copy.wait()
    project_q(0)
    wk_copy.wait()
    wv_copy.wait()
    wo_copy.start()
    project(0)
    pair_copy.wait_recv()
    project_q(1)
    project(1)
    arrive(0)
    attend(0)
    twins(0)
    project(2)
    arrive(1)
    attend(1)
    twins(1)
    project(3)
    attend(2)
    arrive(2)
    attend(3)
    twins(2)
    project(4)
    attend(4, range(0, 3))
    arrive(3)
    attend(4, range(3, 6))
    twins(3)
    project(5)
    attend(5, range(0, 3))
    arrive(4)
    attend(5, range(3, 6))
    twins(4)
    project(6)
    arrive(5)
    attend(6)
    arrive(6)
    twins(5)
    project_first(7)
    twins(6)
    project_second(7)

    def ocopy(i):
        rows = slice(i * half // 2, (i + 1) * half // 2)
        return remote(osend.at[rows, :], oother.at[rows, :], osend_sem, orecv_sem.at[i], partner)

    attend(7, range(0, 3), last=True)
    ocopy(0).start()
    attend(7, range(3, 6), last=True)
    ocopy(1).start()
    wo_copy.wait()
    hh = half // 2

    def wo_rows(start, n):
        return wo[pl.ds(pl.multiple_of(start, HEAD), n), :]

    ocopy(0).wait_recv()
    facc[...] = dot_t(oown[...], wo_rows(core * half, half)) + dot_t(oother[0:hh, :], wo_rows((1 - core) * half, hh))
    ocopy(1).wait_recv()
    y_ref[...] = (facc[...] + dot_t(oother[hh:, :], wo_rows((1 - core) * half + hh, hh))).astype(BF16)

    sent = xbuf.at[0:7]
    remote(sent, sent, send_sem, pair_sem, partner).wait_send()
    remote(osend, osend, osend_sem, pair_sem, partner).wait_send()


def solution(mesh):
    def block(x, w_qkv, w_o):
        tok, width = x.shape[1], x.shape[2]
        half = width // 2
        nh = half // HEAD
        any_spec = pl.BlockSpec(memory_space=pl.ANY)
        dma = pltpu.SemaphoreType.DMA
        y = pl.pallas_call(
            kernel,
            out_shape=jax.ShapeDtypeStruct((tok, width), BF16),
            in_specs=[any_spec] * 3,
            out_specs=pl.BlockSpec(memory_space=pltpu.VMEM),
            scratch_shapes=[
                pltpu.VMEM((8, tok, width), BF16),
                pltpu.VMEM((width, half), BF16),
                pltpu.VMEM((width, half), BF16),
                pltpu.VMEM((width, half), BF16),
                pltpu.VMEM((width, width), BF16),
                pltpu.VMEM((nh, HEAD, 2 * tok), BF16),
                pltpu.VMEM((tok, half), BF16),
                pltpu.VMEM((tok, half), BF16),
                pltpu.VMEM((tok, half), BF16),
                pltpu.VMEM((tok, half), BF16),
                pltpu.VMEM((nh, HEAD, 2 * tok), F32),
                pltpu.VMEM((nh, 1, 2 * tok), F32),
                pltpu.VMEM((nh, 1, 2 * tok), F32),
                pltpu.VMEM((half, tok), BF16),
                pltpu.VMEM((half, tok), BF16),
                pltpu.VMEM((half, tok), BF16),
                pltpu.VMEM((tok, width), F32),
                dma((4,)), dma((2,)), dma(()), dma(()), dma(()), dma((7,)), dma((7,)), dma((2,)),
            ],
            compiler_params=pltpu.CompilerParams(
                collective_id=0, has_side_effects=True, vmem_limit_bytes=53 * 1024 * 1024),
            name="gather_attend",
        )(x[0], w_qkv, w_o.reshape(width, width))
        return y[None]

    return jax.shard_map(
        block, mesh=mesh,
        in_specs=(P("dp", ("cx", "cy"), None), P(None, None), P(None, None, None)),
        out_specs=P("dp", ("cx", "cy"), None), check_vma=False)
```

```python
import math

import jax
import jax.numpy as jnp
from jax import lax
from jax.experimental import pallas as pl
from jax.experimental.pallas import tpu as pltpu
from jax.sharding import PartitionSpec as P

MESH = pl.DeviceIdType.MESH
BF16, F32 = jnp.bfloat16, jnp.float32
HEAD = 128


def kernel(x_hbm, wqkv_hbm, wo_hbm, y_ref,
           xbuf, wq, wk, wv, wo, qt, kbuf0, kbuf1, vbuf0, vbuf1, acc, mrow, lrow, osend, oown, oother, facc,
           w_sem, x_sem, pair_sem, send_sem, osend_sem, link_sem, twin_sem, orecv_sem):
    tok, width = x_hbm.shape
    half = width // 2
    nh = half // HEAD
    quarter = tok // 4
    cut = 9 * HEAD
    scale = math.log2(math.e) / math.sqrt(HEAD)

    dp, cx, cy = lax.axis_index("dp"), lax.axis_index("cx"), lax.axis_index("cy")
    core = lax.rem(cy, 2)
    partner = (dp, cx, cy + 1 - 2 * core)
    xnbr = (dp, cx, lax.rem(cy + 2, 4))
    ynbr = (dp, 1 - cx, cy)

    def wcopy(i, dst):
        cols = pl.ds(pl.multiple_of(i * width + core * half, HEAD), half)
        return pltpu.make_async_copy(wqkv_hbm.at[:, cols], dst, w_sem.at[i])

    wq_copy, wk_copy, wv_copy = wcopy(0, wq), wcopy(1, wk), wcopy(2, wv)
    wo_copy = pltpu.make_async_copy(wo_hbm, wo, w_sem.at[3])

    def own_rows(i, n=1):
        return xbuf.at[0, pl.ds(i * quarter, n * quarter), :]

    for i in (2, 0, 3, 1):
        pltpu.make_async_copy(x_hbm.at[pl.ds(i * quarter, quarter), :], own_rows(i), x_sem.at[i % 2]).start()

    def xload_wait(i):
        pltpu.make_async_copy(x_hbm.at[pl.ds(0, 2 * quarter), :], own_rows(0, 2), x_sem.at[i]).wait()

    barrier = pltpu.get_barrier_semaphore()
    for nbr in (partner, xnbr, ynbr):
        pl.semaphore_signal(barrier, inc=1, device_id=nbr, device_id_type=MESH)
    acc[...] = jnp.zeros_like(acc)
    lrow[...] = jnp.zeros_like(lrow)
    mrow[...] = jnp.full(mrow.shape, -jnp.inf, F32)
    wq_copy.start()
    xload_wait(0)
    pl.semaphore_wait(barrier, 3)

    pieces = [(c, slice(0, width)) for c in range(2, 7)] + [(7, slice(0, cut)), (7, slice(cut, width))]

    def part(c, q, cols):
        return xbuf.at[c, q * quarter:(q + 1) * quarter, cols]

    def remote(src, dst, ssem, rsem, dev):
        return pltpu.make_async_remote_copy(src_ref=src, dst_ref=dst, send_sem=ssem, recv_sem=rsem,
                                            device_id=dev, device_id_type=MESH)

    def link_copy(i, q):
        c, cols = pieces[i]
        dev = xnbr if q == 0 else ynbr
        if c < 6:
            src = own_rows((c if q == 0 else c - 2) % 4)
        else:
            src = part(c - 4, 2 - q, cols)
        return remote(src, part(c, q, cols), send_sem, link_sem.at[i], dev)

    def twin_copy(i, q):
        c, cols = pieces[i]
        return remote(part(c, q, cols), part(c, q + 1, cols), send_sem, twin_sem.at[i], partner)

    pair_copy = remote(xbuf.at[0], xbuf.at[1], send_sem, pair_sem, partner)
    depth = 3

    def send(i):
        if i < len(pieces):
            link_copy(i, 0).start()
            link_copy(i, 2).start()

    def both_parts(i, sems):
        c, cols = pieces[i]
        both = xbuf.at[c, 0:2 * quarter, cols]
        return remote(both, both, send_sem, sems.at[i], partner)

    def arrive(i):
        both_parts(i, link_sem).wait_recv()
        twin_copy(i, 0).start()
        twin_copy(i, 2).start()
        if i == 1:
            send(i + 2)
        send(i + depth - (i < 1))

    def twins(i):
        both_parts(i, twin_sem).wait_recv()

    @pl.when(core == 0)
    def _():
        send(0)

    xload_wait(1)

    @pl.when(core == 0)
    def _():
        send(1)

    pair_copy.start()
    wk_copy.start()
    wv_copy.start()

    def dot(a, b):
        return jnp.dot(a, b, preferred_element_type=F32)

    def dot_t(a, b):
        return lax.dot_general(a, b, (((0,), (0,)), ((), ())), preferred_element_type=F32)

    kbufs, vbufs = (kbuf0, kbuf1), (vbuf0, vbuf1)

    def project_q(c):
        q = dot(xbuf[c], wq[...]).astype(BF16)
        for h in range(nh):
            qt[h, :, c * tok:(c + 1) * tok] = q[:, h * HEAD:(h + 1) * HEAD].T

    def project(c):
        xs = xbuf[c]
        kbufs[c % 2][...] = dot(xs, wk[...]).astype(BF16)
        vbufs[c % 2][...] = dot(xs, wv[...]).astype(BF16)

    def project_first(c):
        xs = xbuf[c, :, 0:cut]
        facc[:, 0:half] = dot(xs, wk[0:cut, :])
        facc[:, half:] = dot(xs, wv[0:cut, :])

    def project_second(c):
        xs = xbuf[c, :, cut:]
        kbufs[c % 2][...] = (facc[:, 0:half] + dot(xs, wk[cut:, :])).astype(BF16)
        vbufs[c % 2][...] = (facc[:, half:] + dot(xs, wv[cut:, :])).astype(BF16)

    def attend(c, heads=range(nh), last=False):
        kb, vb = kbufs[c % 2], vbufs[c % 2]

        def logits(h):
            return dot(kb[:, h * HEAD:(h + 1) * HEAD], qt[h])

        s = logits(heads[0])
        for h in heads:
            s_next = logits(h + 1) if h + 1 in heads else None
            m_old = mrow[h]
            m_new = jnp.maximum(m_old, jnp.max(s, axis=0, keepdims=True))
            p = jnp.exp2((s - m_new) * scale)
            a = jnp.exp2((m_old - m_new) * scale)
            l_new = lrow[h] * a + jnp.sum(p, axis=0, keepdims=True)
            o_new = acc[h] * a + dot_t(vb[:, h * HEAD:(h + 1) * HEAD], p.astype(BF16))
            if not last:
                lrow[h] = l_new
                mrow[h] = m_new
                acc[h] = o_new
            else:
                o = (o_new * (1.0 / l_new)).astype(BF16)
                oown[h * HEAD:(h + 1) * HEAD, :] = o[:, 0:tok]
                osend[h * HEAD:(h + 1) * HEAD, :] = o[:, tok:]
            s = s_next

    wq_copy.wait()

    @pl.when(core == 1)
    def _():
        send(0)
        send(1)

    project_q(0)
    wk_copy.wait()
    wv_copy.wait()
    wo_copy.start()
    project(0)
    pair_copy.wait_recv()
    project_q(1)
    project(1)
    arrive(0)
    attend(0)
    twins(0)
    project(2)
    arrive(1)
    attend(1)
    twins(1)
    project(3)
    attend(2)
    arrive(2)
    attend(3)
    twins(2)
    project(4)
    attend(4, range(0, 3))
    arrive(3)
    attend(4, range(3, 6))
    twins(3)
    project(5)
    attend(5, range(0, 3))
    arrive(4)
    attend(5, range(3, 6))
    twins(4)
    project(6)
    arrive(5)
    attend(6)
    arrive(6)
    twins(5)
    project_first(7)
    twins(6)
    project_second(7)

    def ocopy(i):
        rows = slice(i * half // 2, (i + 1) * half // 2)
        return remote(osend.at[rows, :], oother.at[rows, :], osend_sem, orecv_sem.at[i], partner)

    attend(7, range(0, 3), last=True)
    ocopy(0).start()
    attend(7, range(3, 6), last=True)
    ocopy(1).start()
    wo_copy.wait()
    hh = half // 2

    def wo_rows(start, n):
        return wo[pl.ds(pl.multiple_of(start, HEAD), n), :]

    ocopy(0).wait_recv()
    facc[...] = dot_t(oown[...], wo_rows(core * half, half)) + dot_t(oother[0:hh, :], wo_rows((1 - core) * half, hh))
    ocopy(1).wait_recv()
    y_ref[...] = (facc[...] + dot_t(oother[hh:, :], wo_rows((1 - core) * half + hh, hh))).astype(BF16)

    sent = xbuf.at[0:7]
    remote(sent, sent, send_sem, pair_sem, partner).wait_send()
    remote(osend, osend, osend_sem, pair_sem, partner).wait_send()


def solution(mesh):
    def block(x, w_qkv, w_o):
        tok, width = x.shape[1], x.shape[2]
        half = width // 2
        nh = half // HEAD
        any_spec = pl.BlockSpec(memory_space=pl.ANY)
        dma = pltpu.SemaphoreType.DMA
        y = pl.pallas_call(
            kernel,
            out_shape=jax.ShapeDtypeStruct((tok, width), BF16),
            in_specs=[any_spec] * 3,
            out_specs=pl.BlockSpec(memory_space=pltpu.VMEM),
            scratch_shapes=[
                pltpu.VMEM((8, tok, width), BF16),
                pltpu.VMEM((width, half), BF16),
                pltpu.VMEM((width, half), BF16),
                pltpu.VMEM((width, half), BF16),
                pltpu.VMEM((width, width), BF16),
                pltpu.VMEM((nh, HEAD, 2 * tok), BF16),
                pltpu.VMEM((tok, half), BF16),
                pltpu.VMEM((tok, half), BF16),
                pltpu.VMEM((tok, half), BF16),
                pltpu.VMEM((tok, half), BF16),
                pltpu.VMEM((nh, HEAD, 2 * tok), F32),
                pltpu.VMEM((nh, 1, 2 * tok), F32),
                pltpu.VMEM((nh, 1, 2 * tok), F32),
                pltpu.VMEM((half, tok), BF16),
                pltpu.VMEM((half, tok), BF16),
                pltpu.VMEM((half, tok), BF16),
                pltpu.VMEM((tok, width), F32),
                dma((4,)), dma((2,)), dma(()), dma(()), dma(()), dma((7,)), dma((7,)), dma((2,)),
            ],
            compiler_params=pltpu.CompilerParams(
                collective_id=0, has_side_effects=True, vmem_limit_bytes=53 * 1024 * 1024),
            name="gather_attend",
        )(x[0], w_qkv, w_o.reshape(width, width))
        return y[None]

    return jax.shard_map(
        block, mesh=mesh,
        in_specs=(P("dp", ("cx", "cy"), None), P(None, None), P(None, None, None)),
        out_specs=P("dp", ("cx", "cy"), None), check_vma=False)
```

```python
import math

import jax
import jax.numpy as jnp
from jax import lax
from jax.experimental import pallas as pl
from jax.experimental.pallas import tpu as pltpu
from jax.sharding import PartitionSpec as P

MESH = pl.DeviceIdType.MESH
BF16, F32 = jnp.bfloat16, jnp.float32
HEAD = 128


def kernel(x_hbm, wqkv_hbm, wo_hbm, y_ref,
           xbuf, wq, wk, wv, wo, qt, kbuf0, kbuf1, vbuf0, vbuf1, acc, mrow, lrow, osend, oown, oother, facc,
           w_sem, x_sem, pair_sem, send_sem, osend_sem, link_sem, twin_sem, orecv_sem):
    tok, width = x_hbm.shape
    half = width // 2
    nh = half // HEAD
    quarter = tok // 4
    cut = 9 * HEAD
    scale = math.log2(math.e) / math.sqrt(HEAD)

    dp, cx, cy = lax.axis_index("dp"), lax.axis_index("cx"), lax.axis_index("cy")
    core = lax.rem(cy, 2)
    partner = (dp, cx, cy + 1 - 2 * core)
    xnbr = (dp, cx, lax.rem(cy + 2, 4))
    ynbr = (dp, 1 - cx, cy)

    def wcopy(i, dst):
        cols = pl.ds(pl.multiple_of(i * width + core * half, HEAD), half)
        return pltpu.make_async_copy(wqkv_hbm.at[:, cols], dst, w_sem.at[i])

    wq_copy, wk_copy, wv_copy = wcopy(0, wq), wcopy(1, wk), wcopy(2, wv)
    wo_copy = pltpu.make_async_copy(wo_hbm, wo, w_sem.at[3])

    def own_rows(i, n=1):
        return xbuf.at[0, pl.ds(i * quarter, n * quarter), :]

    for i in (2, 0, 3, 1):
        pltpu.make_async_copy(x_hbm.at[pl.ds(i * quarter, quarter), :], own_rows(i), x_sem.at[i % 2]).start()

    def xload_wait(i):
        pltpu.make_async_copy(x_hbm.at[pl.ds(0, 2 * quarter), :], own_rows(0, 2), x_sem.at[i]).wait()

    barrier = pltpu.get_barrier_semaphore()
    for nbr in (partner, xnbr, ynbr):
        pl.semaphore_signal(barrier, inc=1, device_id=nbr, device_id_type=MESH)
    acc[...] = jnp.zeros_like(acc)
    lrow[...] = jnp.zeros_like(lrow)
    mrow[...] = jnp.full(mrow.shape, -jnp.inf, F32)
    wq_copy.start()
    xload_wait(0)
    pl.semaphore_wait(barrier, 3)

    pieces = [(c, slice(0, width)) for c in range(2, 7)] + [(7, slice(0, cut)), (7, slice(cut, width))]

    def part(c, q, cols):
        return xbuf.at[c, q * quarter:(q + 1) * quarter, cols]

    def remote(src, dst, ssem, rsem, dev):
        return pltpu.make_async_remote_copy(src_ref=src, dst_ref=dst, send_sem=ssem, recv_sem=rsem,
                                            device_id=dev, device_id_type=MESH)

    def link_copy(i, q):
        c, cols = pieces[i]
        dev = xnbr if q == 0 else ynbr
        if c < 6:
            src = own_rows((c if q == 0 else c - 2) % 4)
        else:
            src = part(c - 4, 2 - q, cols)
        return remote(src, part(c, q, cols), send_sem, link_sem.at[i], dev)

    def twin_copy(i, q):
        c, cols = pieces[i]
        return remote(part(c, q, cols), part(c, q + 1, cols), send_sem, twin_sem.at[i], partner)

    pair_copy = remote(xbuf.at[0], xbuf.at[1], send_sem, pair_sem, partner)
    depth = 3

    def send(i):
        if i < len(pieces):
            link_copy(i, 0).start()
            link_copy(i, 2).start()

    def both_parts(i, sems):
        c, cols = pieces[i]
        both = xbuf.at[c, 0:2 * quarter, cols]
        return remote(both, both, send_sem, sems.at[i], partner)

    def arrive(i):
        both_parts(i, link_sem).wait_recv()
        twin_copy(i, 0).start()
        twin_copy(i, 2).start()
        if i == 1:
            send(i + 2)
        send(i + depth - (i < 1))

    def twins(i):
        both_parts(i, twin_sem).wait_recv()

    @pl.when(core == 0)
    def _():
        send(0)

    xload_wait(1)

    @pl.when(core == 0)
    def _():
        send(1)

    @pl.when(core == 1)
    def _():
        pair_copy.start()

    wk_copy.start()
    wv_copy.start()

    def dot(a, b):
        return jnp.dot(a, b, preferred_element_type=F32)

    def dot_t(a, b):
        return lax.dot_general(a, b, (((0,), (0,)), ((), ())), preferred_element_type=F32)

    kbufs, vbufs = (kbuf0, kbuf1), (vbuf0, vbuf1)

    def project_q(c):
        q = dot(xbuf[c], wq[...]).astype(BF16)
        for h in range(nh):
            qt[h, :, c * tok:(c + 1) * tok] = q[:, h * HEAD:(h + 1) * HEAD].T

    def project(c):
        xs = xbuf[c]
        kbufs[c % 2][...] = dot(xs, wk[...]).astype(BF16)
        vbufs[c % 2][...] = dot(xs, wv[...]).astype(BF16)

    def project_first(c):
        xs = xbuf[c, :, 0:cut]
        facc[:, 0:half] = dot(xs, wk[0:cut, :])
        facc[:, half:] = dot(xs, wv[0:cut, :])

    def project_second(c):
        xs = xbuf[c, :, cut:]
        kbufs[c % 2][...] = (facc[:, 0:half] + dot(xs, wk[cut:, :])).astype(BF16)
        vbufs[c % 2][...] = (facc[:, half:] + dot(xs, wv[cut:, :])).astype(BF16)

    def attend(c, heads=range(nh), last=False):
        kb, vb = kbufs[c % 2], vbufs[c % 2]

        def logits(h):
            return dot(kb[:, h * HEAD:(h + 1) * HEAD], qt[h])

        s = logits(heads[0])
        for h in heads:
            s_next = logits(h + 1) if h + 1 in heads else None
            m_old = mrow[h]
            m_new = jnp.maximum(m_old, jnp.max(s, axis=0, keepdims=True))
            p = jnp.exp2((s - m_new) * scale)
            a = jnp.exp2((m_old - m_new) * scale)
            l_new = lrow[h] * a + jnp.sum(p, axis=0, keepdims=True)
            o_new = acc[h] * a + dot_t(vb[:, h * HEAD:(h + 1) * HEAD], p.astype(BF16))
            if not last:
                lrow[h] = l_new
                mrow[h] = m_new
                acc[h] = o_new
            else:
                o = (o_new * (1.0 / l_new)).astype(BF16)
                oown[h * HEAD:(h + 1) * HEAD, :] = o[:, 0:tok]
                osend[h * HEAD:(h + 1) * HEAD, :] = o[:, tok:]
            s = s_next

    wq_copy.wait()

    @pl.when(core == 0)
    def _():
        pair_copy.start()

    @pl.when(core == 1)
    def _():
        send(0)
        send(1)

    project_q(0)
    wk_copy.wait()
    wv_copy.wait()
    wo_copy.start()
    project(0)
    pair_copy.wait_recv()
    project_q(1)
    project(1)
    arrive(0)
    attend(0)
    twins(0)
    project(2)
    arrive(1)
    attend(1)
    twins(1)
    project(3)
    attend(2)
    arrive(2)
    attend(3)
    twins(2)
    project(4)
    attend(4, range(0, 3))
    arrive(3)
    attend(4, range(3, 6))
    twins(3)
    project(5)
    attend(5, range(0, 3))
    arrive(4)
    attend(5, range(3, 6))
    twins(4)
    project(6)
    arrive(5)
    attend(6)
    arrive(6)
    twins(5)
    project_first(7)
    twins(6)
    project_second(7)

    def ocopy(i):
        rows = slice(i * half // 2, (i + 1) * half // 2)
        return remote(osend.at[rows, :], oother.at[rows, :], osend_sem, orecv_sem.at[i], partner)

    attend(7, range(0, 3), last=True)
    ocopy(0).start()
    attend(7, range(3, 6), last=True)
    ocopy(1).start()
    wo_copy.wait()
    hh = half // 2

    def wo_rows(start, n):
        return wo[pl.ds(pl.multiple_of(start, HEAD), n), :]

    ocopy(0).wait_recv()
    facc[...] = dot_t(oown[...], wo_rows(core * half, half)) + dot_t(oother[0:hh, :], wo_rows((1 - core) * half, hh))
    ocopy(1).wait_recv()
    y_ref[...] = (facc[...] + dot_t(oother[hh:, :], wo_rows((1 - core) * half + hh, hh))).astype(BF16)

    sent = xbuf.at[0:7]
    remote(sent, sent, send_sem, pair_sem, partner).wait_send()
    remote(osend, osend, osend_sem, pair_sem, partner).wait_send()


def solution(mesh):
    def block(x, w_qkv, w_o):
        tok, width = x.shape[1], x.shape[2]
        half = width // 2
        nh = half // HEAD
        any_spec = pl.BlockSpec(memory_space=pl.ANY)
        dma = pltpu.SemaphoreType.DMA
        y = pl.pallas_call(
            kernel,
            out_shape=jax.ShapeDtypeStruct((tok, width), BF16),
            in_specs=[any_spec] * 3,
            out_specs=pl.BlockSpec(memory_space=pltpu.VMEM),
            scratch_shapes=[
                pltpu.VMEM((8, tok, width), BF16),
                pltpu.VMEM((width, half), BF16),
                pltpu.VMEM((width, half), BF16),
                pltpu.VMEM((width, half), BF16),
                pltpu.VMEM((width, width), BF16),
                pltpu.VMEM((nh, HEAD, 2 * tok), BF16),
                pltpu.VMEM((tok, half), BF16),
                pltpu.VMEM((tok, half), BF16),
                pltpu.VMEM((tok, half), BF16),
                pltpu.VMEM((tok, half), BF16),
                pltpu.VMEM((nh, HEAD, 2 * tok), F32),
                pltpu.VMEM((nh, 1, 2 * tok), F32),
                pltpu.VMEM((nh, 1, 2 * tok), F32),
                pltpu.VMEM((half, tok), BF16),
                pltpu.VMEM((half, tok), BF16),
                pltpu.VMEM((half, tok), BF16),
                pltpu.VMEM((tok, width), F32),
                dma((4,)), dma((2,)), dma(()), dma(()), dma(()), dma((7,)), dma((7,)), dma((2,)),
            ],
            compiler_params=pltpu.CompilerParams(
                collective_id=0, has_side_effects=True, vmem_limit_bytes=53 * 1024 * 1024),
            name="gather_attend",
        )(x[0], w_qkv, w_o.reshape(width, width))
        return y[None]

    return jax.shard_map(
        block, mesh=mesh,
        in_specs=(P("dp", ("cx", "cy"), None), P(None, None), P(None, None, None)),
        out_specs=P("dp", ("cx", "cy"), None), check_vma=False)
```

```python
import math

import jax
import jax.numpy as jnp
from jax import lax
from jax.experimental import pallas as pl
from jax.experimental.pallas import tpu as pltpu
from jax.sharding import PartitionSpec as P

MESH = pl.DeviceIdType.MESH
BF16, F32 = jnp.bfloat16, jnp.float32
HEAD = 128


def kernel(x_hbm, wqkv_hbm, wo_hbm, y_ref,
           xbuf, wq, wk, wv, wo, qt, kbuf0, kbuf1, vbuf0, vbuf1, acc, mrow, lrow, osend, oown, oother, facc,
           w_sem, x_sem, pair_sem, send_sem, osend_sem, link_sem, twin_sem, orecv_sem):
    tok, width = x_hbm.shape
    half = width // 2
    nh = half // HEAD
    quarter = tok // 4
    cut = 9 * HEAD
    scale = math.log2(math.e) / math.sqrt(HEAD)

    dp, cx, cy = lax.axis_index("dp"), lax.axis_index("cx"), lax.axis_index("cy")
    core = lax.rem(cy, 2)
    partner = (dp, cx, cy + 1 - 2 * core)
    xnbr = (dp, cx, lax.rem(cy + 2, 4))
    ynbr = (dp, 1 - cx, cy)

    def wcopy(i, dst):
        cols = pl.ds(pl.multiple_of(i * width + core * half, HEAD), half)
        return pltpu.make_async_copy(wqkv_hbm.at[:, cols], dst, w_sem.at[i])

    wq_copy, wk_copy, wv_copy = wcopy(0, wq), wcopy(1, wk), wcopy(2, wv)
    wo_copy = pltpu.make_async_copy(wo_hbm, wo, w_sem.at[3])

    def own_rows(i, n=1):
        return xbuf.at[0, pl.ds(i * quarter, n * quarter), :]

    for i in (2, 0, 3, 1):
        pltpu.make_async_copy(x_hbm.at[pl.ds(i * quarter, quarter), :], own_rows(i), x_sem.at[i % 2]).start()

    def xload_wait(i):
        pltpu.make_async_copy(x_hbm.at[pl.ds(0, 2 * quarter), :], own_rows(0, 2), x_sem.at[i]).wait()

    barrier = pltpu.get_barrier_semaphore()
    for nbr in (partner, xnbr, ynbr):
        pl.semaphore_signal(barrier, inc=1, device_id=nbr, device_id_type=MESH)
    acc[...] = jnp.zeros_like(acc)
    lrow[...] = jnp.zeros_like(lrow)
    mrow[...] = jnp.full(mrow.shape, -jnp.inf, F32)
    wq_copy.start()
    xload_wait(0)
    pl.semaphore_wait(barrier, 3)

    pieces = [(c, slice(0, width)) for c in range(2, 7)] + [(7, slice(0, cut)), (7, slice(cut, width))]

    def part(c, q, cols):
        return xbuf.at[c, q * quarter:(q + 1) * quarter, cols]

    def remote(src, dst, ssem, rsem, dev):
        return pltpu.make_async_remote_copy(src_ref=src, dst_ref=dst, send_sem=ssem, recv_sem=rsem,
                                            device_id=dev, device_id_type=MESH)

    def link_copy(i, q):
        c, cols = pieces[i]
        dev = xnbr if q == 0 else ynbr
        if c < 6:
            src = own_rows((c if q == 0 else c - 2) % 4)
        else:
            src = part(c - 4, 1 - q, cols)
        return remote(src, part(c, q, cols), send_sem, link_sem.at[i], dev)

    def twin_copy(i, q):
        c, cols = pieces[i]
        return remote(part(c, q, cols), part(c, q + 2, cols), send_sem, twin_sem.at[i], partner)

    pair_copy = remote(xbuf.at[0], xbuf.at[1], send_sem, pair_sem, partner)
    depth = 3

    def send(i):
        if i < len(pieces):
            link_copy(i, 0).start()
            link_copy(i, 1).start()

    def both_parts(i, sems):
        c, cols = pieces[i]
        both = xbuf.at[c, 0:2 * quarter, cols]
        return remote(both, both, send_sem, sems.at[i], partner)

    def arrive(i):
        both_parts(i, link_sem).wait_recv()
        twin_copy(i, 0).start()
        twin_copy(i, 1).start()
        if i == 1:
            send(i + 2)
        send(i + depth - (i < 1))

    def twins(i):
        both_parts(i, twin_sem).wait_recv()

    send(0)
    xload_wait(1)
    send(1)
    pair_copy.start()
    wk_copy.start()
    wv_copy.start()

    def dot(a, b):
        return jnp.dot(a, b, preferred_element_type=F32)

    def dot_t(a, b):
        return lax.dot_general(a, b, (((0,), (0,)), ((), ())), preferred_element_type=F32)

    kbufs, vbufs = (kbuf0, kbuf1), (vbuf0, vbuf1)

    def project_q(c):
        q = dot(xbuf[c], wq[...]).astype(BF16)
        for h in range(nh):
            qt[h, :, c * tok:(c + 1) * tok] = q[:, h * HEAD:(h + 1) * HEAD].T

    def project(c, lo=0, hi=tok):
        xs = xbuf[c, lo:hi, :]
        kbufs[c % 2][lo:hi, :] = dot(xs, wk[...]).astype(BF16)
        vbufs[c % 2][lo:hi, :] = dot(xs, wv[...]).astype(BF16)

    def project_first(c):
        xs = xbuf[c, :, 0:cut]
        facc[:, 0:half] = dot(xs, wk[0:cut, :])
        facc[:, half:] = dot(xs, wv[0:cut, :])

    def project_second(c):
        xs = xbuf[c, :, cut:]
        kbufs[c % 2][...] = (facc[:, 0:half] + dot(xs, wk[cut:, :])).astype(BF16)
        vbufs[c % 2][...] = (facc[:, half:] + dot(xs, wv[cut:, :])).astype(BF16)

    def attend(c, heads=range(nh), last=False):
        kb, vb = kbufs[c % 2], vbufs[c % 2]

        def logits(h):
            return dot(kb[:, h * HEAD:(h + 1) * HEAD], qt[h])

        s = logits(heads[0])
        for h in heads:
            s_next = logits(h + 1) if h + 1 in heads else None
            m_old = mrow[h]
            m_new = jnp.maximum(m_old, jnp.max(s, axis=0, keepdims=True))
            p = jnp.exp2((s - m_new) * scale)
            a = jnp.exp2((m_old - m_new) * scale)
            l_new = lrow[h] * a + jnp.sum(p, axis=0, keepdims=True)
            o_new = acc[h] * a + dot_t(vb[:, h * HEAD:(h + 1) * HEAD], p.astype(BF16))
            if not last:
                lrow[h] = l_new
                mrow[h] = m_new
                acc[h] = o_new
            else:
                o = (o_new * (1.0 / l_new)).astype(BF16)
                oown[h * HEAD:(h + 1) * HEAD, :] = o[:, 0:tok]
                osend[h * HEAD:(h + 1) * HEAD, :] = o[:, tok:]
            s = s_next

    wq_copy.wait()
    project_q(0)
    wk_copy.wait()
    wv_copy.wait()
    wo_copy.start()
    project(0)
    pair_copy.wait_recv()
    project_q(1)
    project(1)
    arrive(0)
    attend(0)
    twins(0)
    project(2)
    arrive(1)
    attend(1)
    twins(1)
    project(3)
    attend(2)
    arrive(2)
    attend(3)
    twins(2)
    project(4)
    attend(4, range(0, 3))
    arrive(3)
    attend(4, range(3, 6))
    twins(3)
    project(5)
    attend(5, range(0, 3))
    arrive(4)
    project(6, 0, tok // 2)
    attend(5, range(3, 6))
    twins(4)
    project(6, tok // 2, tok)
    arrive(5)
    attend(6)
    arrive(6)
    twins(5)
    project_first(7)
    twins(6)
    project_second(7)

    first = 4

    def ocopy(i):
        rows = slice(0, first * HEAD) if i == 0 else slice(first * HEAD, half)
        return remote(osend.at[rows, :], oother.at[rows, :], osend_sem, orecv_sem.at[i], partner)

    attend(7, range(0, first), last=True)
    ocopy(0).start()
    attend(7, range(first, nh), last=True)
    ocopy(1).start()
    wo_copy.wait()

    def wo_rows(start, n):
        return wo[pl.ds(pl.multiple_of(start, HEAD), n), :]

    cutrow = first * HEAD
    other = (1 - core) * half
    facc[...] = dot_t(oown[...], wo_rows(core * half, half))
    ocopy(0).wait_recv()
    facc[...] += dot_t(oother[0:cutrow, :], wo_rows(other, cutrow))
    ocopy(1).wait_recv()
    y_ref[...] = (facc[...] + dot_t(oother[cutrow:, :], wo_rows(other + cutrow, half - cutrow))).astype(BF16)

    sent = xbuf.at[0:7]
    remote(sent, sent, send_sem, pair_sem, partner).wait_send()
    remote(osend, osend, osend_sem, pair_sem, partner).wait_send()


def solution(mesh):
    def block(x, w_qkv, w_o):
        tok, width = x.shape[1], x.shape[2]
        half = width // 2
        nh = half // HEAD
        any_spec = pl.BlockSpec(memory_space=pl.ANY)
        dma = pltpu.SemaphoreType.DMA
        y = pl.pallas_call(
            kernel,
            out_shape=jax.ShapeDtypeStruct((tok, width), BF16),
            in_specs=[any_spec] * 3,
            out_specs=pl.BlockSpec(memory_space=pltpu.VMEM),
            scratch_shapes=[
                pltpu.VMEM((8, tok, width), BF16),
                pltpu.VMEM((width, half), BF16),
                pltpu.VMEM((width, half), BF16),
                pltpu.VMEM((width, half), BF16),
                pltpu.VMEM((width, width), BF16),
                pltpu.VMEM((nh, HEAD, 2 * tok), BF16),
                pltpu.VMEM((tok, half), BF16),
                pltpu.VMEM((tok, half), BF16),
                pltpu.VMEM((tok, half), BF16),
                pltpu.VMEM((tok, half), BF16),
                pltpu.VMEM((nh, HEAD, 2 * tok), F32),
                pltpu.VMEM((nh, 1, 2 * tok), F32),
                pltpu.VMEM((nh, 1, 2 * tok), F32),
                pltpu.VMEM((half, tok), BF16),
                pltpu.VMEM((half, tok), BF16),
                pltpu.VMEM((half, tok), BF16),
                pltpu.VMEM((tok, width), F32),
                dma((4,)), dma((2,)), dma(()), dma(()), dma(()), dma((7,)), dma((7,)), dma((2,)),
            ],
            compiler_params=pltpu.CompilerParams(
                collective_id=0, has_side_effects=True, vmem_limit_bytes=53 * 1024 * 1024),
            name="gather_attend",
        )(x[0], w_qkv, w_o.reshape(width, width))
        return y[None]

    return jax.shard_map(
        block, mesh=mesh,
        in_specs=(P("dp", ("cx", "cy"), None), P(None, None), P(None, None, None)),
        out_specs=P("dp", ("cx", "cy"), None), check_vma=False)
```

```python
import math

import jax
import jax.numpy as jnp
from jax import lax
from jax.experimental import pallas as pl
from jax.experimental.pallas import tpu as pltpu
from jax.sharding import PartitionSpec as P

MESH = pl.DeviceIdType.MESH
BF16, F32 = jnp.bfloat16, jnp.float32
HEAD = 128


def kernel(x_hbm, wqkv_hbm, wo_hbm, y_ref,
           xbuf, wq, wk, wv, wo, qt, kbuf0, kbuf1, vbuf0, vbuf1, acc, mrow, lrow, osend, oown, oother, facc,
           w_sem, x_sem, pair_sem, send_sem, osend_sem, link_sem, twin_sem, orecv_sem):
    tok, width = x_hbm.shape
    half = width // 2
    nh = half // HEAD
    quarter = tok // 4
    cut = 9 * HEAD
    scale = math.log2(math.e) / math.sqrt(HEAD)

    dp, cx, cy = lax.axis_index("dp"), lax.axis_index("cx"), lax.axis_index("cy")
    core = lax.rem(cy, 2)
    partner = (dp, cx, cy + 1 - 2 * core)
    xnbr = (dp, cx, lax.rem(cy + 2, 4))
    ynbr = (dp, 1 - cx, cy)

    def wcopy(i, dst):
        cols = pl.ds(pl.multiple_of(i * width + core * half, HEAD), half)
        return pltpu.make_async_copy(wqkv_hbm.at[:, cols], dst, w_sem.at[i])

    wq_copy, wk_copy, wv_copy = wcopy(0, wq), wcopy(1, wk), wcopy(2, wv)
    wo_copy = pltpu.make_async_copy(wo_hbm, wo, w_sem.at[3])

    def own_rows(i, n=1):
        return xbuf.at[0, pl.ds(i * quarter, n * quarter), :]

    for i in (2, 0, 3, 1):
        pltpu.make_async_copy(x_hbm.at[pl.ds(i * quarter, quarter), :], own_rows(i), x_sem.at[i % 2]).start()

    def xload_wait(i):
        pltpu.make_async_copy(x_hbm.at[pl.ds(0, 2 * quarter), :], own_rows(0, 2), x_sem.at[i]).wait()

    barrier = pltpu.get_barrier_semaphore()
    for nbr in (partner, xnbr, ynbr):
        pl.semaphore_signal(barrier, inc=1, device_id=nbr, device_id_type=MESH)
    acc[...] = jnp.zeros_like(acc)
    lrow[...] = jnp.zeros_like(lrow)
    mrow[...] = jnp.full(mrow.shape, -jnp.inf, F32)
    wq_copy.start()
    xload_wait(0)
    pl.semaphore_wait(barrier, 3)

    pieces = [(c, slice(0, width)) for c in range(2, 7)] + [(7, slice(0, cut)), (7, slice(cut, width))]

    def part(c, q, cols):
        return xbuf.at[c, q * quarter:(q + 1) * quarter, cols]

    def remote(src, dst, ssem, rsem, dev):
        return pltpu.make_async_remote_copy(src_ref=src, dst_ref=dst, send_sem=ssem, recv_sem=rsem,
                                            device_id=dev, device_id_type=MESH)

    def link_copy(i, q):
        c, cols = pieces[i]
        dev = xnbr if q == 0 else ynbr
        if c < 6:
            src = own_rows((c if q == 0 else c - 2) % 4)
        else:
            src = part(c - 4, 1 - q, cols)
        return remote(src, part(c, q, cols), send_sem, link_sem.at[i], dev)

    def twin_copies(i):
        c, cols = pieces[i]
        n = 2 * quarter // 8
        for r in range(8):
            src = xbuf.at[c, r * n:(r + 1) * n, cols]
            dst = xbuf.at[c, 2 * quarter + r * n:2 * quarter + (r + 1) * n, cols]
            remote(src, dst, send_sem, twin_sem.at[i], partner).start()

    pair_copy = remote(xbuf.at[0], xbuf.at[1], send_sem, pair_sem, partner)
    depth = 3

    def send(i):
        if i < len(pieces):
            link_copy(i, 0).start()
            link_copy(i, 1).start()

    def both_parts(i, sems):
        c, cols = pieces[i]
        both = xbuf.at[c, 0:2 * quarter, cols]
        return remote(both, both, send_sem, sems.at[i], partner)

    def arrive(i):
        both_parts(i, link_sem).wait_recv()
        twin_copies(i)
        if i == 1:
            send(i + 2)
        send(i + depth - (i < 1))

    def twins(i):
        both_parts(i, twin_sem).wait_recv()

    send(0)
    xload_wait(1)
    send(1)
    pair_copy.start()
    wk_copy.start()
    wv_copy.start()

    def dot(a, b):
        return jnp.dot(a, b, preferred_element_type=F32)

    def dot_t(a, b):
        return lax.dot_general(a, b, (((0,), (0,)), ((), ())), preferred_element_type=F32)

    kbufs, vbufs = (kbuf0, kbuf1), (vbuf0, vbuf1)

    def project_q(c):
        q = dot(xbuf[c], wq[...]).astype(BF16)
        for h in range(nh):
            qt[h, :, c * tok:(c + 1) * tok] = q[:, h * HEAD:(h + 1) * HEAD].T

    def project(c, lo=0, hi=tok):
        xs = xbuf[c, lo:hi, :]
        kbufs[c % 2][lo:hi, :] = dot(xs, wk[...]).astype(BF16)
        vbufs[c % 2][lo:hi, :] = dot(xs, wv[...]).astype(BF16)

    def project_first(c):
        xs = xbuf[c, :, 0:cut]
        facc[:, 0:half] = dot(xs, wk[0:cut, :])
        facc[:, half:] = dot(xs, wv[0:cut, :])

    def project_second(c):
        xs = xbuf[c, :, cut:]
        kbufs[c % 2][...] = (facc[:, 0:half] + dot(xs, wk[cut:, :])).astype(BF16)
        vbufs[c % 2][...] = (facc[:, half:] + dot(xs, wv[cut:, :])).astype(BF16)

    def attend(c, heads=range(nh), last=False):
        kb, vb = kbufs[c % 2], vbufs[c % 2]

        def logits(h):
            return dot(kb[:, h * HEAD:(h + 1) * HEAD], qt[h])

        s = logits(heads[0])
        for h in heads:
            s_next = logits(h + 1) if h + 1 in heads else None
            m_old = mrow[h]
            m_new = jnp.maximum(m_old, jnp.max(s, axis=0, keepdims=True))
            p = jnp.exp2((s - m_new) * scale)
            a = jnp.exp2((m_old - m_new) * scale)
            l_new = lrow[h] * a + jnp.sum(p, axis=0, keepdims=True)
            o_new = acc[h] * a + dot_t(vb[:, h * HEAD:(h + 1) * HEAD], p.astype(BF16))
            if not last:
                lrow[h] = l_new
                mrow[h] = m_new
                acc[h] = o_new
            else:
                o = (o_new * (1.0 / l_new)).astype(BF16)
                oown[h * HEAD:(h + 1) * HEAD, :] = o[:, 0:tok]
                osend[h * HEAD:(h + 1) * HEAD, :] = o[:, tok:]
            s = s_next

    wq_copy.wait()
    project_q(0)
    wk_copy.wait()
    wv_copy.wait()
    wo_copy.start()
    project(0)
    pair_copy.wait_recv()
    project_q(1)
    project(1)
    arrive(0)
    attend(0)
    twins(0)
    project(2)
    arrive(1)
    attend(1)
    twins(1)
    project(3)
    attend(2)
    arrive(2)
    attend(3)
    twins(2)
    project(4)
    attend(4, range(0, 3))
    arrive(3)
    attend(4, range(3, 6))
    twins(3)
    project(5)
    attend(5, range(0, 3))
    arrive(4)
    project(6, 0, tok // 2)
    attend(5, range(3, 6))
    twins(4)
    project(6, tok // 2, tok)
    arrive(5)
    attend(6)
    arrive(6)
    twins(5)
    project_first(7)
    twins(6)
    project_second(7)

    first = 4

    def ocopy(i):
        rows = slice(0, first * HEAD) if i == 0 else slice(first * HEAD, half)
        return remote(osend.at[rows, :], oother.at[rows, :], osend_sem, orecv_sem.at[i], partner)

    attend(7, range(0, first), last=True)
    ocopy(0).start()
    attend(7, range(first, nh), last=True)
    ocopy(1).start()
    wo_copy.wait()

    def wo_rows(start, n):
        return wo[pl.ds(pl.multiple_of(start, HEAD), n), :]

    cutrow = first * HEAD
    other = (1 - core) * half
    facc[...] = dot_t(oown[...], wo_rows(core * half, half))
    ocopy(0).wait_recv()
    facc[...] += dot_t(oother[0:cutrow, :], wo_rows(other, cutrow))
    ocopy(1).wait_recv()
    y_ref[...] = (facc[...] + dot_t(oother[cutrow:, :], wo_rows(other + cutrow, half - cutrow))).astype(BF16)

    sent = xbuf.at[0:7]
    remote(sent, sent, send_sem, pair_sem, partner).wait_send()
    remote(osend, osend, osend_sem, pair_sem, partner).wait_send()


def solution(mesh):
    def block(x, w_qkv, w_o):
        tok, width = x.shape[1], x.shape[2]
        half = width // 2
        nh = half // HEAD
        any_spec = pl.BlockSpec(memory_space=pl.ANY)
        dma = pltpu.SemaphoreType.DMA
        y = pl.pallas_call(
            kernel,
            out_shape=jax.ShapeDtypeStruct((tok, width), BF16),
            in_specs=[any_spec] * 3,
            out_specs=pl.BlockSpec(memory_space=pltpu.VMEM),
            scratch_shapes=[
                pltpu.VMEM((8, tok, width), BF16),
                pltpu.VMEM((width, half), BF16),
                pltpu.VMEM((width, half), BF16),
                pltpu.VMEM((width, half), BF16),
                pltpu.VMEM((width, width), BF16),
                pltpu.VMEM((nh, HEAD, 2 * tok), BF16),
                pltpu.VMEM((tok, half), BF16),
                pltpu.VMEM((tok, half), BF16),
                pltpu.VMEM((tok, half), BF16),
                pltpu.VMEM((tok, half), BF16),
                pltpu.VMEM((nh, HEAD, 2 * tok), F32),
                pltpu.VMEM((nh, 1, 2 * tok), F32),
                pltpu.VMEM((nh, 1, 2 * tok), F32),
                pltpu.VMEM((half, tok), BF16),
                pltpu.VMEM((half, tok), BF16),
                pltpu.VMEM((half, tok), BF16),
                pltpu.VMEM((tok, width), F32),
                dma((4,)), dma((2,)), dma(()), dma(()), dma(()), dma((7,)), dma((7,)), dma((2,)),
            ],
            compiler_params=pltpu.CompilerParams(
                collective_id=0, has_side_effects=True, vmem_limit_bytes=53 * 1024 * 1024),
            name="gather_attend",
        )(x[0], w_qkv, w_o.reshape(width, width))
        return y[None]

    return jax.shard_map(
        block, mesh=mesh,
        in_specs=(P("dp", ("cx", "cy"), None), P(None, None), P(None, None, None)),
        out_specs=P("dp", ("cx", "cy"), None), check_vma=False)
```

```python
import math

import jax
import jax.numpy as jnp
from jax import lax
from jax.experimental import pallas as pl
from jax.experimental.pallas import tpu as pltpu
from jax.sharding import PartitionSpec as P

MESH = pl.DeviceIdType.MESH
BF16, F32 = jnp.bfloat16, jnp.float32
HEAD = 128


def kernel(x_hbm, wqkv_hbm, wo_hbm, y_ref,
           xbuf, wq, wk, wv, wo, qt, kbuf0, kbuf1, vbuf0, vbuf1, acc, mrow, lrow, osend, oown, oother, facc, sbuf,
           w_sem, x_sem, pair_sem, send_sem, osend_sem, link_sem, twin_sem, orecv_sem):
    tok, width = x_hbm.shape
    half = width // 2
    nh = half // HEAD
    quarter = tok // 4
    cut = 9 * HEAD
    scale = math.log2(math.e) / math.sqrt(HEAD)

    dp, cx, cy = lax.axis_index("dp"), lax.axis_index("cx"), lax.axis_index("cy")
    core = lax.rem(cy, 2)
    partner = (dp, cx, cy + 1 - 2 * core)
    xnbr = (dp, cx, lax.rem(cy + 2, 4))
    ynbr = (dp, 1 - cx, cy)

    def wcopy(i, dst):
        cols = pl.ds(pl.multiple_of(i * width + core * half, HEAD), half)
        return pltpu.make_async_copy(wqkv_hbm.at[:, cols], dst, w_sem.at[i])

    wq_copy, wk_copy, wv_copy = wcopy(0, wq), wcopy(1, wk), wcopy(2, wv)
    wo_copy = pltpu.make_async_copy(wo_hbm, wo, w_sem.at[3])

    def own_rows(i, n=1):
        return xbuf.at[0, pl.ds(i * quarter, n * quarter), :]

    for i in (2, 0, 3, 1):
        pltpu.make_async_copy(x_hbm.at[pl.ds(i * quarter, quarter), :], own_rows(i), x_sem.at[i % 2]).start()

    def xload_wait(i):
        pltpu.make_async_copy(x_hbm.at[pl.ds(0, 2 * quarter), :], own_rows(0, 2), x_sem.at[i]).wait()

    barrier = pltpu.get_barrier_semaphore()
    for nbr in (partner, xnbr, ynbr):
        pl.semaphore_signal(barrier, inc=1, device_id=nbr, device_id_type=MESH)
    acc[...] = jnp.zeros_like(acc)
    lrow[...] = jnp.zeros_like(lrow)
    mrow[...] = jnp.full(mrow.shape, -jnp.inf, F32)
    wq_copy.start()
    xload_wait(0)
    pl.semaphore_wait(barrier, 3)

    pieces = [(c, slice(0, width)) for c in range(2, 7)] + [(7, slice(0, cut)), (7, slice(cut, width))]

    def part(c, q, cols):
        return xbuf.at[c, q * quarter:(q + 1) * quarter, cols]

    def remote(src, dst, ssem, rsem, dev):
        return pltpu.make_async_remote_copy(src_ref=src, dst_ref=dst, send_sem=ssem, recv_sem=rsem,
                                            device_id=dev, device_id_type=MESH)

    def link_copy(i, q):
        c, cols = pieces[i]
        dev = xnbr if q == 0 else ynbr
        if c < 6:
            src = own_rows((c if q == 0 else c - 2) % 4)
        else:
            src = part(c - 4, 1 - q, cols)
        return remote(src, part(c, q, cols), send_sem, link_sem.at[i], dev)

    def twin_copy(i, q):
        c, cols = pieces[i]
        return remote(part(c, q, cols), part(c, q + 2, cols), send_sem, twin_sem.at[i], partner)

    pair_copy = remote(xbuf.at[0], xbuf.at[1], send_sem, pair_sem, partner)
    depth = 3

    def send(i):
        if i < len(pieces):
            link_copy(i, 0).start()
            link_copy(i, 1).start()

    def both_parts(i, sems):
        c, cols = pieces[i]
        both = xbuf.at[c, 0:2 * quarter, cols]
        return remote(both, both, send_sem, sems.at[i], partner)

    def arrive(i):
        both_parts(i, link_sem).wait_recv()
        twin_copy(i, 0).start()
        twin_copy(i, 1).start()
        if i == 1:
            send(i + 2)
        send(i + depth - (i < 1))

    def twins(i):
        both_parts(i, twin_sem).wait_recv()

    send(0)
    xload_wait(1)
    send(1)
    pair_copy.start()
    wk_copy.start()
    wv_copy.start()

    def dot(a, b):
        return jnp.dot(a, b, preferred_element_type=F32)

    def dot_t(a, b):
        return lax.dot_general(a, b, (((0,), (0,)), ((), ())), preferred_element_type=F32)

    kbufs, vbufs = (kbuf0, kbuf1), (vbuf0, vbuf1)

    def project_q(c):
        q = dot(xbuf[c], wq[...]).astype(BF16)
        for h in range(nh):
            qt[h, :, c * tok:(c + 1) * tok] = q[:, h * HEAD:(h + 1) * HEAD].T

    def project(c, lo=0, hi=tok):
        xs = xbuf[c, lo:hi, :]
        kbufs[c % 2][lo:hi, :] = dot(xs, wk[...]).astype(BF16)
        vbufs[c % 2][lo:hi, :] = dot(xs, wv[...]).astype(BF16)

    def project_first(c):
        xs = xbuf[c, :, 0:cut]
        facc[:, 0:half] = dot(xs, wk[0:cut, :])
        facc[:, half:] = dot(xs, wv[0:cut, :])

    def project_second(c):
        xs = xbuf[c, :, cut:]
        kbufs[c % 2][...] = (facc[:, 0:half] + dot(xs, wk[cut:, :])).astype(BF16)
        vbufs[c % 2][...] = (facc[:, half:] + dot(xs, wv[cut:, :])).astype(BF16)

    def attend(c, heads=range(nh), last=False):
        kb, vb = kbufs[c % 2], vbufs[c % 2]

        for h in heads:
            sbuf[h] = dot(kb[:, h * HEAD:(h + 1) * HEAD], qt[h])
        for h in heads:
            s = sbuf[h]
            m_old = mrow[h]
            m_new = jnp.maximum(m_old, jnp.max(s, axis=0, keepdims=True))
            p = jnp.exp2((s - m_new) * scale)
            a = jnp.exp2((m_old - m_new) * scale)
            l_new = lrow[h] * a + jnp.sum(p, axis=0, keepdims=True)
            o_new = acc[h] * a + dot_t(vb[:, h * HEAD:(h + 1) * HEAD], p.astype(BF16))
            if not last:
                lrow[h] = l_new
                mrow[h] = m_new
                acc[h] = o_new
            else:
                o = (o_new * (1.0 / l_new)).astype(BF16)
                oown[h * HEAD:(h + 1) * HEAD, :] = o[:, 0:tok]
                osend[h * HEAD:(h + 1) * HEAD, :] = o[:, tok:]

    wq_copy.wait()
    project_q(0)
    wk_copy.wait()
    wv_copy.wait()
    wo_copy.start()
    project(0)
    pair_copy.wait_recv()
    project_q(1)
    project(1)
    arrive(0)
    attend(0)
    twins(0)
    project(2)
    arrive(1)
    attend(1)
    twins(1)
    project(3)
    attend(2)
    arrive(2)
    attend(3)
    twins(2)
    project(4)
    attend(4, range(0, 3))
    arrive(3)
    attend(4, range(3, 6))
    twins(3)
    project(5)
    attend(5, range(0, 3))
    arrive(4)
    project(6, 0, tok // 2)
    attend(5, range(3, 6))
    twins(4)
    project(6, tok // 2, tok)
    arrive(5)
    attend(6)
    arrive(6)
    twins(5)
    project_first(7)
    twins(6)
    project_second(7)

    first = 4

    def ocopy(i):
        rows = slice(0, first * HEAD) if i == 0 else slice(first * HEAD, half)
        return remote(osend.at[rows, :], oother.at[rows, :], osend_sem, orecv_sem.at[i], partner)

    attend(7, range(0, first), last=True)
    ocopy(0).start()
    attend(7, range(first, nh), last=True)
    ocopy(1).start()
    wo_copy.wait()

    def wo_rows(start, n):
        return wo[pl.ds(pl.multiple_of(start, HEAD), n), :]

    cutrow = first * HEAD
    other = (1 - core) * half
    facc[...] = dot_t(oown[...], wo_rows(core * half, half))
    ocopy(0).wait_recv()
    facc[...] += dot_t(oother[0:cutrow, :], wo_rows(other, cutrow))
    ocopy(1).wait_recv()
    y_ref[...] = (facc[...] + dot_t(oother[cutrow:, :], wo_rows(other + cutrow, half - cutrow))).astype(BF16)

    sent = xbuf.at[0:7]
    remote(sent, sent, send_sem, pair_sem, partner).wait_send()
    remote(osend, osend, osend_sem, pair_sem, partner).wait_send()


def solution(mesh):
    def block(x, w_qkv, w_o):
        tok, width = x.shape[1], x.shape[2]
        half = width // 2
        nh = half // HEAD
        any_spec = pl.BlockSpec(memory_space=pl.ANY)
        dma = pltpu.SemaphoreType.DMA
        y = pl.pallas_call(
            kernel,
            out_shape=jax.ShapeDtypeStruct((tok, width), BF16),
            in_specs=[any_spec] * 3,
            out_specs=pl.BlockSpec(memory_space=pltpu.VMEM),
            scratch_shapes=[
                pltpu.VMEM((8, tok, width), BF16),
                pltpu.VMEM((width, half), BF16),
                pltpu.VMEM((width, half), BF16),
                pltpu.VMEM((width, half), BF16),
                pltpu.VMEM((width, width), BF16),
                pltpu.VMEM((nh, HEAD, 2 * tok), BF16),
                pltpu.VMEM((tok, half), BF16),
                pltpu.VMEM((tok, half), BF16),
                pltpu.VMEM((tok, half), BF16),
                pltpu.VMEM((tok, half), BF16),
                pltpu.VMEM((nh, HEAD, 2 * tok), F32),
                pltpu.VMEM((nh, 1, 2 * tok), F32),
                pltpu.VMEM((nh, 1, 2 * tok), F32),
                pltpu.VMEM((half, tok), BF16),
                pltpu.VMEM((half, tok), BF16),
                pltpu.VMEM((half, tok), BF16),
                pltpu.VMEM((tok, width), F32),
                pltpu.VMEM((nh, tok, 2 * tok), F32),
                dma((4,)), dma((2,)), dma(()), dma(()), dma(()), dma((7,)), dma((7,)), dma((2,)),
            ],
            compiler_params=pltpu.CompilerParams(
                collective_id=0, has_side_effects=True, vmem_limit_bytes=53 * 1024 * 1024),
            name="gather_attend",
        )(x[0], w_qkv, w_o.reshape(width, width))
        return y[None]

    return jax.shard_map(
        block, mesh=mesh,
        in_specs=(P("dp", ("cx", "cy"), None), P(None, None), P(None, None, None)),
        out_specs=P("dp", ("cx", "cy"), None), check_vma=False)
```

```python
import math

import jax
import jax.numpy as jnp
from jax import lax
from jax.experimental import pallas as pl
from jax.experimental.pallas import tpu as pltpu
from jax.sharding import PartitionSpec as P

MESH = pl.DeviceIdType.MESH
BF16, F32 = jnp.bfloat16, jnp.float32
HEAD = 128


def kernel(x_hbm, wqkv_hbm, wo_hbm, y_ref,
           xbuf, wq, wk, wv, wo, qt, kbuf0, kbuf1, vbuf0, vbuf1, acc, mrow, lrow, osend, oown, oother, facc, sbuf,
           w_sem, x_sem, pair_sem, send_sem, osend_sem, link_sem, twin_sem, orecv_sem):
    tok, width = x_hbm.shape
    half = width // 2
    nh = half // HEAD
    quarter = tok // 4
    cut = 8 * HEAD
    scale = math.log2(math.e) / math.sqrt(HEAD)

    dp, cx, cy = lax.axis_index("dp"), lax.axis_index("cx"), lax.axis_index("cy")
    core = lax.rem(cy, 2)
    partner = (dp, cx, cy + 1 - 2 * core)
    xnbr = (dp, cx, lax.rem(cy + 2, 4))
    ynbr = (dp, 1 - cx, cy)

    def wcopy(i, dst):
        cols = pl.ds(pl.multiple_of(i * width + core * half, HEAD), half)
        return pltpu.make_async_copy(wqkv_hbm.at[:, cols], dst, w_sem.at[i])

    wq_copy, wk_copy, wv_copy = wcopy(0, wq), wcopy(1, wk), wcopy(2, wv)
    wo_copy = pltpu.make_async_copy(wo_hbm, wo, w_sem.at[3])

    def own_rows(i, n=1):
        return xbuf.at[0, pl.ds(i * quarter, n * quarter), :]

    for i in (2, 0, 3, 1):
        pltpu.make_async_copy(x_hbm.at[pl.ds(i * quarter, quarter), :], own_rows(i), x_sem.at[i % 2]).start()

    def xload_wait(i):
        pltpu.make_async_copy(x_hbm.at[pl.ds(0, 2 * quarter), :], own_rows(0, 2), x_sem.at[i]).wait()

    barrier = pltpu.get_barrier_semaphore()
    for nbr in (partner, xnbr, ynbr):
        pl.semaphore_signal(barrier, inc=1, device_id=nbr, device_id_type=MESH)
    acc[...] = jnp.zeros_like(acc)
    lrow[...] = jnp.zeros_like(lrow)
    mrow[...] = jnp.full(mrow.shape, -jnp.inf, F32)
    wq_copy.start()
    xload_wait(0)
    pl.semaphore_wait(barrier, 3)

    pieces = [(c, slice(0, width)) for c in range(2, 7)] + [(7, slice(0, cut)), (7, slice(cut, width))]

    def part(c, q, cols):
        return xbuf.at[c, q * quarter:(q + 1) * quarter, cols]

    def remote(src, dst, ssem, rsem, dev):
        return pltpu.make_async_remote_copy(src_ref=src, dst_ref=dst, send_sem=ssem, recv_sem=rsem,
                                            device_id=dev, device_id_type=MESH)

    def link_copy(i, q):
        c, cols = pieces[i]
        dev = xnbr if q == 0 else ynbr
        if c < 6:
            src = own_rows((c if q == 0 else c - 2) % 4)
        else:
            src = part(c - 4, 1 - q, cols)
        return remote(src, part(c, q, cols), send_sem, link_sem.at[i], dev)

    def twin_copy(i, q):
        c, cols = pieces[i]
        return remote(part(c, q, cols), part(c, q + 2, cols), send_sem, twin_sem.at[i], partner)

    pair_copy = remote(xbuf.at[0], xbuf.at[1], send_sem, pair_sem, partner)
    depth = 3

    def send(i):
        if i < len(pieces):
            link_copy(i, 0).start()
            link_copy(i, 1).start()

    def both_parts(i, sems):
        c, cols = pieces[i]
        both = xbuf.at[c, 0:2 * quarter, cols]
        return remote(both, both, send_sem, sems.at[i], partner)

    def arrive(i):
        both_parts(i, link_sem).wait_recv()
        twin_copy(i, 0).start()
        twin_copy(i, 1).start()
        if i == 1:
            send(i + 2)
        send(i + depth - (i < 1))

    def twins(i):
        both_parts(i, twin_sem).wait_recv()

    send(0)
    xload_wait(1)
    send(1)
    pair_copy.start()
    wk_copy.start()
    wv_copy.start()

    def dot(a, b):
        return jnp.dot(a, b, preferred_element_type=F32)

    def dot_t(a, b):
        return lax.dot_general(a, b, (((0,), (0,)), ((), ())), preferred_element_type=F32)

    kbufs, vbufs = (kbuf0, kbuf1), (vbuf0, vbuf1)

    def project_q(c):
        q = dot(xbuf[c], wq[...]).astype(BF16)
        for h in range(nh):
            qt[h, :, c * tok:(c + 1) * tok] = q[:, h * HEAD:(h + 1) * HEAD].T

    def project(c, lo=0, hi=tok):
        xs = xbuf[c, lo:hi, :]
        kbufs[c % 2][lo:hi, :] = dot(xs, wk[...]).astype(BF16)
        vbufs[c % 2][lo:hi, :] = dot(xs, wv[...]).astype(BF16)

    def project_first(c):
        xs = xbuf[c, :, 0:cut]
        facc[:, 0:half] = dot(xs, wk[0:cut, :])
        facc[:, half:] = dot(xs, wv[0:cut, :])

    def project_second(c, lo, hi):
        xs = xbuf[c, lo:hi, cut:]
        kbufs[c % 2][lo:hi, :] = (facc[lo:hi, 0:half] + dot(xs, wk[cut:, :])).astype(BF16)
        vbufs[c % 2][lo:hi, :] = (facc[lo:hi, half:] + dot(xs, wv[cut:, :])).astype(BF16)

    def attend(c, heads=range(nh), last=False):
        kb, vb = kbufs[c % 2], vbufs[c % 2]

        for h in heads:
            sbuf[h] = dot(kb[:, h * HEAD:(h + 1) * HEAD], qt[h])
        for h in heads:
            s = sbuf[h]
            m_old = mrow[h]
            m_new = jnp.maximum(m_old, jnp.max(s, axis=0, keepdims=True))
            p = jnp.exp2((s - m_new) * scale)
            a = jnp.exp2((m_old - m_new) * scale)
            l_new = lrow[h] * a + jnp.sum(p, axis=0, keepdims=True)
            o_new = acc[h] * a + dot_t(vb[:, h * HEAD:(h + 1) * HEAD], p.astype(BF16))
            if not last:
                lrow[h] = l_new
                mrow[h] = m_new
                acc[h] = o_new
            else:
                o = (o_new * (1.0 / l_new)).astype(BF16)
                oown[h * HEAD:(h + 1) * HEAD, :] = o[:, 0:tok]
                osend[h * HEAD:(h + 1) * HEAD, :] = o[:, tok:]

    wq_copy.wait()
    project_q(0)
    wk_copy.wait()
    wv_copy.wait()
    wo_copy.start()
    project(0)
    pair_copy.wait_recv()
    project_q(1)
    project(1)
    arrive(0)
    attend(0)
    twins(0)
    project(2)
    arrive(1)
    attend(1)
    twins(1)
    project(3)
    attend(2)
    arrive(2)
    attend(3)
    twins(2)
    project(4)
    attend(4, range(0, 3))
    arrive(3)
    attend(4, range(3, 6))
    twins(3)
    project(5)
    attend(5)
    arrive(4)
    project(6, 0, tok // 2)
    twins(4)
    project(6, tok // 2, tok)
    arrive(5)
    attend(6)
    arrive(6)
    twins(5)
    project_first(7)
    project_second(7, 0, tok // 2)
    twins(6)
    project_second(7, tok // 2, tok)

    first = 5

    def ocopy(i):
        rows = slice(0, first * HEAD) if i == 0 else slice(first * HEAD, half)
        return remote(osend.at[rows, :], oother.at[rows, :], osend_sem, orecv_sem.at[i], partner)

    attend(7, range(0, first), last=True)
    ocopy(0).start()
    attend(7, range(first, nh), last=True)
    ocopy(1).start()
    wo_copy.wait()

    def wo_rows(start, n):
        return wo[pl.ds(pl.multiple_of(start, HEAD), n), :]

    cutrow = first * HEAD
    other = (1 - core) * half
    facc[...] = dot_t(oown[...], wo_rows(core * half, half))
    ocopy(0).wait_recv()
    facc[...] += dot_t(oother[0:cutrow, :], wo_rows(other, cutrow))
    ocopy(1).wait_recv()
    y_ref[...] = (facc[...] + dot_t(oother[cutrow:, :], wo_rows(other + cutrow, half - cutrow))).astype(BF16)

    sent = xbuf.at[0:7]
    remote(sent, sent, send_sem, pair_sem, partner).wait_send()
    remote(osend, osend, osend_sem, pair_sem, partner).wait_send()


def solution(mesh):
    def block(x, w_qkv, w_o):
        tok, width = x.shape[1], x.shape[2]
        half = width // 2
        nh = half // HEAD
        any_spec = pl.BlockSpec(memory_space=pl.ANY)
        dma = pltpu.SemaphoreType.DMA
        y = pl.pallas_call(
            kernel,
            out_shape=jax.ShapeDtypeStruct((tok, width), BF16),
            in_specs=[any_spec] * 3,
            out_specs=pl.BlockSpec(memory_space=pltpu.VMEM),
            scratch_shapes=[
                pltpu.VMEM((8, tok, width), BF16),
                pltpu.VMEM((width, half), BF16),
                pltpu.VMEM((width, half), BF16),
                pltpu.VMEM((width, half), BF16),
                pltpu.VMEM((width, width), BF16),
                pltpu.VMEM((nh, HEAD, 2 * tok), BF16),
                pltpu.VMEM((tok, half), BF16),
                pltpu.VMEM((tok, half), BF16),
                pltpu.VMEM((tok, half), BF16),
                pltpu.VMEM((tok, half), BF16),
                pltpu.VMEM((nh, HEAD, 2 * tok), F32),
                pltpu.VMEM((nh, 1, 2 * tok), F32),
                pltpu.VMEM((nh, 1, 2 * tok), F32),
                pltpu.VMEM((half, tok), BF16),
                pltpu.VMEM((half, tok), BF16),
                pltpu.VMEM((half, tok), BF16),
                pltpu.VMEM((tok, width), F32),
                pltpu.VMEM((nh, tok, 2 * tok), F32),
                dma((4,)), dma((2,)), dma(()), dma(()), dma(()), dma((7,)), dma((7,)), dma((2,)),
            ],
            compiler_params=pltpu.CompilerParams(
                collective_id=0, has_side_effects=True, vmem_limit_bytes=53 * 1024 * 1024),
            name="gather_attend",
        )(x[0], w_qkv, w_o.reshape(width, width))
        return y[None]

    return jax.shard_map(
        block, mesh=mesh,
        in_specs=(P("dp", ("cx", "cy"), None), P(None, None), P(None, None, None)),
        out_specs=P("dp", ("cx", "cy"), None), check_vma=False)
```

```python
import math

import jax
import jax.numpy as jnp
from jax import lax
from jax.experimental import pallas as pl
from jax.experimental.pallas import tpu as pltpu
from jax.sharding import PartitionSpec as P

MESH = pl.DeviceIdType.MESH
BF16, F32 = jnp.bfloat16, jnp.float32
HEAD = 128


def kernel(x_hbm, wqkv_hbm, wo_hbm, y_ref,
           xbuf, wq, wk, wv, wo, qt, kbuf0, kbuf1, vbuf0, vbuf1, acc, mrow, lrow, osend, oown, oother, facc, sbuf,
           w_sem, x_sem, pair_sem, send_sem, osend_sem, link_sem, twin_sem, orecv_sem):
    tok, width = x_hbm.shape
    half = width // 2
    nh = half // HEAD
    quarter = tok // 4
    cut = 9 * HEAD
    scale = math.log2(math.e) / math.sqrt(HEAD)

    dp, cx, cy = lax.axis_index("dp"), lax.axis_index("cx"), lax.axis_index("cy")
    core = lax.rem(cy, 2)
    partner = (dp, cx, cy + 1 - 2 * core)
    xnbr = (dp, cx, lax.rem(cy + 2, 4))
    ynbr = (dp, 1 - cx, cy)

    def wcopy(i, dst):
        cols = pl.ds(pl.multiple_of(i * width + core * half, HEAD), half)
        return pltpu.make_async_copy(wqkv_hbm.at[:, cols], dst, w_sem.at[i])

    wq_copy, wk_copy, wv_copy = wcopy(0, wq), wcopy(1, wk), wcopy(2, wv)
    wo_copy = pltpu.make_async_copy(wo_hbm, wo, w_sem.at[3])

    def own_rows(i, n=1):
        return xbuf.at[0, pl.ds(i * quarter, n * quarter), :]

    def xload(i):
        pltpu.make_async_copy(x_hbm.at[pl.ds(i * quarter, quarter), :], own_rows(i), x_sem.at[i % 2]).start()

    xload(2)
    xload(0)

    def xload_wait(i):
        pltpu.make_async_copy(x_hbm.at[pl.ds(0, 2 * quarter), :], own_rows(0, 2), x_sem.at[i]).wait()

    barrier = pltpu.get_barrier_semaphore()
    for nbr in (partner, xnbr, ynbr):
        pl.semaphore_signal(barrier, inc=1, device_id=nbr, device_id_type=MESH)
    acc[...] = jnp.zeros_like(acc)
    lrow[...] = jnp.zeros_like(lrow)
    mrow[...] = jnp.full(mrow.shape, -jnp.inf, F32)
    xload_wait(0)
    xload(3)
    xload(1)
    wq_copy.start()
    pl.semaphore_wait(barrier, 3)

    pieces = [(c, slice(0, width)) for c in range(2, 7)] + [(7, slice(0, cut)), (7, slice(cut, width))]

    def part(c, q, cols):
        return xbuf.at[c, q * quarter:(q + 1) * quarter, cols]

    def remote(src, dst, ssem, rsem, dev):
        return pltpu.make_async_remote_copy(src_ref=src, dst_ref=dst, send_sem=ssem, recv_sem=rsem,
                                            device_id=dev, device_id_type=MESH)

    def link_copy(i, q):
        c, cols = pieces[i]
        dev = xnbr if q == 0 else ynbr
        if c < 6:
            src = own_rows((c if q == 0 else c - 2) % 4)
        else:
            src = part(c - 4, 1 - q, cols)
        return remote(src, part(c, q, cols), send_sem, link_sem.at[i], dev)

    def twin_copy(i, q):
        c, cols = pieces[i]
        return remote(part(c, q, cols), part(c, q + 2, cols), send_sem, twin_sem.at[i], partner)

    pair_copy = remote(xbuf.at[0], xbuf.at[1], send_sem, pair_sem, partner)
    depth = 3

    def send(i):
        if i < len(pieces):
            link_copy(i, 0).start()
            link_copy(i, 1).start()

    def both_parts(i, sems):
        c, cols = pieces[i]
        both = xbuf.at[c, 0:2 * quarter, cols]
        return remote(both, both, send_sem, sems.at[i], partner)

    def arrive(i):
        both_parts(i, link_sem).wait_recv()
        twin_copy(i, 0).start()
        twin_copy(i, 1).start()
        if i == 1:
            send(i + 2)
        send(i + depth - (i < 1))

    def twins(i):
        both_parts(i, twin_sem).wait_recv()

    send(0)
    xload_wait(1)
    send(1)
    pair_copy.start()
    wk_copy.start()
    wv_copy.start()

    def dot(a, b):
        return jnp.dot(a, b, preferred_element_type=F32)

    def dot_t(a, b):
        return lax.dot_general(a, b, (((0,), (0,)), ((), ())), preferred_element_type=F32)

    kbufs, vbufs = (kbuf0, kbuf1), (vbuf0, vbuf1)

    def project_q(c):
        q = dot(xbuf[c], wq[...]).astype(BF16)
        for h in range(nh):
            qt[h, :, c * tok:(c + 1) * tok] = q[:, h * HEAD:(h + 1) * HEAD].T

    def project(c, lo=0, hi=tok):
        xs = xbuf[c, lo:hi, :]
        kbufs[c % 2][lo:hi, :] = dot(xs, wk[...]).astype(BF16)
        vbufs[c % 2][lo:hi, :] = dot(xs, wv[...]).astype(BF16)

    def project_first(c):
        xs = xbuf[c, :, 0:cut]
        facc[:, 0:half] = dot(xs, wk[0:cut, :])
        facc[:, half:] = dot(xs, wv[0:cut, :])

    def project_second(c):
        xs = xbuf[c, :, cut:]
        kbufs[c % 2][...] = (facc[:, 0:half] + dot(xs, wk[cut:, :])).astype(BF16)
        vbufs[c % 2][...] = (facc[:, half:] + dot(xs, wv[cut:, :])).astype(BF16)

    def attend(c, heads=range(nh), last=False):
        kb, vb = kbufs[c % 2], vbufs[c % 2]

        for h in heads:
            sbuf[h] = dot(kb[:, h * HEAD:(h + 1) * HEAD], qt[h])
        for h in heads:
            s = sbuf[h]
            m_old = mrow[h]
            m_new = jnp.maximum(m_old, jnp.max(s, axis=0, keepdims=True))
            p = jnp.exp2((s - m_new) * scale)
            a = jnp.exp2((m_old - m_new) * scale)
            l_new = lrow[h] * a + jnp.sum(p, axis=0, keepdims=True)
            o_new = acc[h] * a + dot_t(vb[:, h * HEAD:(h + 1) * HEAD], p.astype(BF16))
            if not last:
                lrow[h] = l_new
                mrow[h] = m_new
                acc[h] = o_new
            else:
                o = (o_new * (1.0 / l_new)).astype(BF16)
                oown[h * HEAD:(h + 1) * HEAD, :] = o[:, 0:tok]
                osend[h * HEAD:(h + 1) * HEAD, :] = o[:, tok:]

    wq_copy.wait()
    project_q(0)
    wk_copy.wait()
    wv_copy.wait()
    wo_copy.start()
    project(0)
    pair_copy.wait_recv()
    project_q(1)
    project(1)
    arrive(0)
    attend(0)
    twins(0)
    project(2)
    arrive(1)
    attend(1)
    twins(1)
    project(3)
    attend(2)
    arrive(2)
    attend(3)
    twins(2)
    project(4)
    attend(4, range(0, 3))
    arrive(3)
    attend(4, range(3, 6))
    twins(3)
    project(5)
    attend(5, range(0, 3))
    arrive(4)
    project(6, 0, tok // 2)
    attend(5, range(3, 6))
    twins(4)
    project(6, tok // 2, tok)
    arrive(5)
    attend(6)
    arrive(6)
    twins(5)
    project_first(7)
    twins(6)
    project_second(7)

    first = 4

    def ocopy(i):
        rows = slice(0, first * HEAD) if i == 0 else slice(first * HEAD, half)
        return remote(osend.at[rows, :], oother.at[rows, :], osend_sem, orecv_sem.at[i], partner)

    attend(7, range(0, first), last=True)
    ocopy(0).start()
    attend(7, range(first, nh), last=True)
    ocopy(1).start()
    wo_copy.wait()

    def wo_rows(start, n):
        return wo[pl.ds(pl.multiple_of(start, HEAD), n), :]

    cutrow = first * HEAD
    other = (1 - core) * half
    facc[...] = dot_t(oown[...], wo_rows(core * half, half))
    ocopy(0).wait_recv()
    facc[...] += dot_t(oother[0:cutrow, :], wo_rows(other, cutrow))
    ocopy(1).wait_recv()
    y_ref[...] = (facc[...] + dot_t(oother[cutrow:, :], wo_rows(other + cutrow, half - cutrow))).astype(BF16)

    sent = xbuf.at[0:7]
    remote(sent, sent, send_sem, pair_sem, partner).wait_send()
    remote(osend, osend, osend_sem, pair_sem, partner).wait_send()


def solution(mesh):
    def block(x, w_qkv, w_o):
        tok, width = x.shape[1], x.shape[2]
        half = width // 2
        nh = half // HEAD
        any_spec = pl.BlockSpec(memory_space=pl.ANY)
        dma = pltpu.SemaphoreType.DMA
        y = pl.pallas_call(
            kernel,
            out_shape=jax.ShapeDtypeStruct((tok, width), BF16),
            in_specs=[any_spec] * 3,
            out_specs=pl.BlockSpec(memory_space=pltpu.VMEM),
            scratch_shapes=[
                pltpu.VMEM((8, tok, width), BF16),
                pltpu.VMEM((width, half), BF16),
                pltpu.VMEM((width, half), BF16),
                pltpu.VMEM((width, half), BF16),
                pltpu.VMEM((width, width), BF16),
                pltpu.VMEM((nh, HEAD, 2 * tok), BF16),
                pltpu.VMEM((tok, half), BF16),
                pltpu.VMEM((tok, half), BF16),
                pltpu.VMEM((tok, half), BF16),
                pltpu.VMEM((tok, half), BF16),
                pltpu.VMEM((nh, HEAD, 2 * tok), F32),
                pltpu.VMEM((nh, 1, 2 * tok), F32),
                pltpu.VMEM((nh, 1, 2 * tok), F32),
                pltpu.VMEM((half, tok), BF16),
                pltpu.VMEM((half, tok), BF16),
                pltpu.VMEM((half, tok), BF16),
                pltpu.VMEM((tok, width), F32),
                pltpu.VMEM((nh, tok, 2 * tok), F32),
                dma((4,)), dma((2,)), dma(()), dma(()), dma(()), dma((7,)), dma((7,)), dma((2,)),
            ],
            compiler_params=pltpu.CompilerParams(
                collective_id=0, has_side_effects=True, vmem_limit_bytes=53 * 1024 * 1024),
            name="gather_attend",
        )(x[0], w_qkv, w_o.reshape(width, width))
        return y[None]

    return jax.shard_map(
        block, mesh=mesh,
        in_specs=(P("dp", ("cx", "cy"), None), P(None, None), P(None, None, None)),
        out_specs=P("dp", ("cx", "cy"), None), check_vma=False)
```

```python
import math

import jax
import jax.numpy as jnp
from jax import lax
from jax.experimental import pallas as pl
from jax.experimental.pallas import tpu as pltpu
from jax.sharding import PartitionSpec as P

MESH = pl.DeviceIdType.MESH
BF16, F32 = jnp.bfloat16, jnp.float32
HEAD = 128


def kernel(x_hbm, wqkv_hbm, wo_hbm, y_ref,
           xbuf, wq, wk, wv, wo, qt, kbuf0, kbuf1, vbuf0, vbuf1, acc, mrow, lrow, osend, oown, oother, facc, sbuf,
           w_sem, x_sem, pair_sem, send_sem, osend_sem, link_sem, twin_sem, orecv_sem):
    tok, width = x_hbm.shape
    half = width // 2
    nh = half // HEAD
    quarter = tok // 4
    cut = 8 * HEAD
    scale = math.log2(math.e) / math.sqrt(HEAD)

    dp, cx, cy = lax.axis_index("dp"), lax.axis_index("cx"), lax.axis_index("cy")
    core = lax.rem(cy, 2)
    partner = (dp, cx, cy + 1 - 2 * core)
    xnbr = (dp, cx, lax.rem(cy + 2, 4))
    ynbr = (dp, 1 - cx, cy)

    def wcopy(i, dst):
        cols = pl.ds(pl.multiple_of(i * width + core * half, HEAD), half)
        return pltpu.make_async_copy(wqkv_hbm.at[:, cols], dst, w_sem.at[i])

    wq_copy, wk_copy, wv_copy = wcopy(0, wq), wcopy(1, wk), wcopy(2, wv)
    wo_copy = pltpu.make_async_copy(wo_hbm, wo, w_sem.at[3])

    def own_rows(i, n=1):
        return xbuf.at[0, pl.ds(i * quarter, n * quarter), :]

    for i in (2, 0, 3, 1):
        pltpu.make_async_copy(x_hbm.at[pl.ds(i * quarter, quarter), :], own_rows(i), x_sem.at[i % 2]).start()

    def xload_wait(i):
        pltpu.make_async_copy(x_hbm.at[pl.ds(0, 2 * quarter), :], own_rows(0, 2), x_sem.at[i]).wait()

    barrier = pltpu.get_barrier_semaphore()
    for nbr in (partner, xnbr, ynbr):
        pl.semaphore_signal(barrier, inc=1, device_id=nbr, device_id_type=MESH)
    acc[...] = jnp.zeros_like(acc)
    lrow[...] = jnp.zeros_like(lrow)
    mrow[...] = jnp.full(mrow.shape, -jnp.inf, F32)
    wq_copy.start()
    xload_wait(0)
    pl.semaphore_wait(barrier, 3)

    pieces = [(c, slice(0, width)) for c in range(2, 7)] + [(7, slice(0, cut)), (7, slice(cut, width))]

    def part(c, q, cols):
        return xbuf.at[c, q * quarter:(q + 1) * quarter, cols]

    def remote(src, dst, ssem, rsem, dev):
        return pltpu.make_async_remote_copy(src_ref=src, dst_ref=dst, send_sem=ssem, recv_sem=rsem,
                                            device_id=dev, device_id_type=MESH)

    def link_copy(i, q):
        c, cols = pieces[i]
        dev = xnbr if q == 0 else ynbr
        if c < 6:
            src = own_rows((c if q == 0 else c - 2) % 4)
        else:
            src = part(c - 4, 1 - q, cols)
        return remote(src, part(c, q, cols), send_sem, link_sem.at[i], dev)

    def twin_copy(i, q):
        c, cols = pieces[i]
        return remote(part(c, q, cols), part(c, q + 2, cols), send_sem, twin_sem.at[i], partner)

    pair_copy = remote(xbuf.at[0], xbuf.at[1], send_sem, pair_sem, partner)
    depth = 3

    def send(i):
        if i < len(pieces):
            link_copy(i, 0).start()
            link_copy(i, 1).start()

    def both_parts(i, sems):
        c, cols = pieces[i]
        both = xbuf.at[c, 0:2 * quarter, cols]
        return remote(both, both, send_sem, sems.at[i], partner)

    def arrive(i):
        both_parts(i, link_sem).wait_recv()
        twin_copy(i, 0).start()
        twin_copy(i, 1).start()
        if i == 1:
            send(i + 2)
        send(i + depth - (i < 1))

    def twins(i):
        both_parts(i, twin_sem).wait_recv()

    send(0)
    xload_wait(1)
    send(1)
    pair_copy.start()
    wk_copy.start()
    wv_copy.start()

    def dot(a, b):
        return jnp.dot(a, b, preferred_element_type=F32)

    def dot_t(a, b):
        return lax.dot_general(a, b, (((0,), (0,)), ((), ())), preferred_element_type=F32)

    kbufs, vbufs = (kbuf0, kbuf1), (vbuf0, vbuf1)

    def project_q(c):
        q = dot(xbuf[c], wq[...]).astype(BF16)
        for h in range(nh):
            qt[h, :, c * tok:(c + 1) * tok] = q[:, h * HEAD:(h + 1) * HEAD].T

    def project(c, lo=0, hi=tok):
        xs = xbuf[c, lo:hi, :]
        kbufs[c % 2][lo:hi, :] = dot(xs, wk[...]).astype(BF16)
        vbufs[c % 2][lo:hi, :] = dot(xs, wv[...]).astype(BF16)

    def project_first(c):
        xs = xbuf[c, :, 0:cut]
        facc[:, 0:half] = dot(xs, wk[0:cut, :])
        facc[:, half:] = dot(xs, wv[0:cut, :])

    def project_second(c, lo, hi):
        xs = xbuf[c, lo:hi, cut:]
        kbufs[c % 2][lo:hi, :] = (facc[lo:hi, 0:half] + dot(xs, wk[cut:, :])).astype(BF16)
        vbufs[c % 2][lo:hi, :] = (facc[lo:hi, half:] + dot(xs, wv[cut:, :])).astype(BF16)

    def attend(c, heads=range(nh), last=False):
        kb, vb = kbufs[c % 2], vbufs[c % 2]

        for h in heads:
            sbuf[h] = dot(kb[:, h * HEAD:(h + 1) * HEAD], qt[h])
        for h in heads:
            s = sbuf[h]
            m_old = mrow[h]
            m_new = jnp.maximum(m_old, jnp.max(s, axis=0, keepdims=True))
            p = jnp.exp2((s - m_new) * scale)
            a = jnp.exp2((m_old - m_new) * scale)
            l_new = lrow[h] * a + jnp.sum(p, axis=0, keepdims=True)
            o_new = acc[h] * a + dot_t(vb[:, h * HEAD:(h + 1) * HEAD], p.astype(BF16))
            if not last:
                lrow[h] = l_new
                mrow[h] = m_new
                acc[h] = o_new
            else:
                o = (o_new * (1.0 / l_new)).astype(BF16)
                oown[h * HEAD:(h + 1) * HEAD, :] = o[:, 0:tok]
                osend[h * HEAD:(h + 1) * HEAD, :] = o[:, tok:]

    wq_copy.wait()
    project_q(0)
    wk_copy.wait()
    wv_copy.wait()
    wo_copy.start()
    project(0)
    pair_copy.wait_recv()
    project_q(1)
    project(1)
    arrive(0)
    attend(0)
    twins(0)
    project(2)
    arrive(1)
    attend(1)
    twins(1)
    project(3)
    attend(2)
    arrive(2)
    attend(3)
    twins(2)
    project(4)
    attend(4, range(0, 3))
    arrive(3)
    attend(4, range(3, 6))
    twins(3)
    project(5)
    attend(5)
    arrive(4)
    project(6, 0, tok // 2)
    twins(4)
    project(6, tok // 2, tok)
    arrive(5)
    attend(6)
    arrive(6)
    twins(5)
    project_first(7)
    project_second(7, 0, tok // 2)
    twins(6)
    project_second(7, tok // 2, tok)

    first = 4

    def ocopy(i):
        rows = slice(0, first * HEAD) if i == 0 else slice(first * HEAD, half)
        return remote(osend.at[rows, :], oother.at[rows, :], osend_sem, orecv_sem.at[i], partner)

    attend(7, range(0, first), last=True)
    ocopy(0).start()
    attend(7, range(first, nh), last=True)
    ocopy(1).start()
    wo_copy.wait()

    def wo_rows(start, n):
        return wo[pl.ds(pl.multiple_of(start, HEAD), n), :]

    cutrow = first * HEAD
    other = (1 - core) * half
    facc[...] = dot_t(oown[...], wo_rows(core * half, half))
    ocopy(0).wait_recv()
    facc[...] += dot_t(oother[0:cutrow, :], wo_rows(other, cutrow))
    ocopy(1).wait_recv()
    y_ref[...] = (facc[...] + dot_t(oother[cutrow:, :], wo_rows(other + cutrow, half - cutrow))).astype(BF16)

    sent = xbuf.at[0:7]
    remote(sent, sent, send_sem, pair_sem, partner).wait_send()
    remote(osend, osend, osend_sem, pair_sem, partner).wait_send()


def solution(mesh):
    def block(x, w_qkv, w_o):
        tok, width = x.shape[1], x.shape[2]
        half = width // 2
        nh = half // HEAD
        any_spec = pl.BlockSpec(memory_space=pl.ANY)
        dma = pltpu.SemaphoreType.DMA
        y = pl.pallas_call(
            kernel,
            out_shape=jax.ShapeDtypeStruct((tok, width), BF16),
            in_specs=[any_spec] * 3,
            out_specs=pl.BlockSpec(memory_space=pltpu.VMEM),
            scratch_shapes=[
                pltpu.VMEM((8, tok, width), BF16),
                pltpu.VMEM((width, half), BF16),
                pltpu.VMEM((width, half), BF16),
                pltpu.VMEM((width, half), BF16),
                pltpu.VMEM((width, width), BF16),
                pltpu.VMEM((nh, HEAD, 2 * tok), BF16),
                pltpu.VMEM((tok, half), BF16),
                pltpu.VMEM((tok, half), BF16),
                pltpu.VMEM((tok, half), BF16),
                pltpu.VMEM((tok, half), BF16),
                pltpu.VMEM((nh, HEAD, 2 * tok), F32),
                pltpu.VMEM((nh, 1, 2 * tok), F32),
                pltpu.VMEM((nh, 1, 2 * tok), F32),
                pltpu.VMEM((half, tok), BF16),
                pltpu.VMEM((half, tok), BF16),
                pltpu.VMEM((half, tok), BF16),
                pltpu.VMEM((tok, width), F32),
                pltpu.VMEM((nh, tok, 2 * tok), F32),
                dma((4,)), dma((2,)), dma(()), dma(()), dma(()), dma((7,)), dma((7,)), dma((2,)),
            ],
            compiler_params=pltpu.CompilerParams(
                collective_id=0, has_side_effects=True, vmem_limit_bytes=53 * 1024 * 1024),
            name="gather_attend",
        )(x[0], w_qkv, w_o.reshape(width, width))
        return y[None]

    return jax.shard_map(
        block, mesh=mesh,
        in_specs=(P("dp", ("cx", "cy"), None), P(None, None), P(None, None, None)),
        out_specs=P("dp", ("cx", "cy"), None), check_vma=False)
```

```python
import math

import jax
import jax.numpy as jnp
from jax import lax
from jax.experimental import pallas as pl
from jax.experimental.pallas import tpu as pltpu
from jax.sharding import PartitionSpec as P

MESH = pl.DeviceIdType.MESH
BF16, F32 = jnp.bfloat16, jnp.float32
HEAD = 128


def kernel(x_hbm, wqkv_hbm, wo_hbm, y_ref,
           xbuf, wq, wk, wv, wo, qt, kbuf0, kbuf1, vbuf0, vbuf1, acc, mrow, lrow, osend, oown, oother, facc, sbuf,
           w_sem, x_sem, pair_sem, send_sem, osend_sem, link_sem, twin_sem, orecv_sem):
    tok, width = x_hbm.shape
    half = width // 2
    nh = half // HEAD
    quarter = tok // 4
    cut = 8 * HEAD
    scale = math.log2(math.e) / math.sqrt(HEAD)

    dp, cx, cy = lax.axis_index("dp"), lax.axis_index("cx"), lax.axis_index("cy")
    core = lax.rem(cy, 2)
    partner = (dp, cx, cy + 1 - 2 * core)
    xnbr = (dp, cx, lax.rem(cy + 2, 4))
    ynbr = (dp, 1 - cx, cy)

    def wcopy(i, dst):
        cols = pl.ds(pl.multiple_of(i * width + core * half, HEAD), half)
        return pltpu.make_async_copy(wqkv_hbm.at[:, cols], dst, w_sem.at[i])

    wq_copy, wk_copy, wv_copy = wcopy(0, wq), wcopy(1, wk), wcopy(2, wv)
    wo_copy = pltpu.make_async_copy(wo_hbm, wo, w_sem.at[3])

    def own_rows(i, n=1):
        return xbuf.at[0, pl.ds(i * quarter, n * quarter), :]

    for i in (2, 0, 3, 1):
        pltpu.make_async_copy(x_hbm.at[pl.ds(i * quarter, quarter), :], own_rows(i), x_sem.at[i % 2]).start()

    def xload_wait(i):
        pltpu.make_async_copy(x_hbm.at[pl.ds(0, 2 * quarter), :], own_rows(0, 2), x_sem.at[i]).wait()

    barrier = pltpu.get_barrier_semaphore()
    for nbr in (partner, xnbr, ynbr):
        pl.semaphore_signal(barrier, inc=1, device_id=nbr, device_id_type=MESH)
    acc[...] = jnp.zeros_like(acc)
    lrow[...] = jnp.zeros_like(lrow)
    mrow[...] = jnp.full(mrow.shape, -jnp.inf, F32)
    wq_copy.start()
    xload_wait(0)
    pl.semaphore_wait(barrier, 3)

    pieces = [(c, slice(0, width)) for c in range(2, 7)] + [(7, slice(0, cut)), (7, slice(cut, width))]

    def part(c, q, cols):
        return xbuf.at[c, q * quarter:(q + 1) * quarter, cols]

    def remote(src, dst, ssem, rsem, dev):
        return pltpu.make_async_remote_copy(src_ref=src, dst_ref=dst, send_sem=ssem, recv_sem=rsem,
                                            device_id=dev, device_id_type=MESH)

    def link_copy(i, q):
        c, cols = pieces[i]
        dev = xnbr if q == 0 else ynbr
        if c < 6:
            src = own_rows((c if q == 0 else c - 2) % 4)
        else:
            src = part(c - 4, 1 - q, cols)
        return remote(src, part(c, q, cols), send_sem, link_sem.at[i], dev)

    def twin_copy(i, q):
        c, cols = pieces[i]
        return remote(part(c, q, cols), part(c, q + 2, cols), send_sem, twin_sem.at[i], partner)

    pair_copy = remote(xbuf.at[0], xbuf.at[1], send_sem, pair_sem, partner)
    depth = 3

    def send(i):
        if i < len(pieces):
            link_copy(i, 0).start()
            link_copy(i, 1).start()

    def both_parts(i, sems):
        c, cols = pieces[i]
        both = xbuf.at[c, 0:2 * quarter, cols]
        return remote(both, both, send_sem, sems.at[i], partner)

    def arrive(i):
        both_parts(i, link_sem).wait_recv()
        twin_copy(i, 0).start()
        twin_copy(i, 1).start()
        if i == 1:
            send(i + 2)
        send(i + depth - (i < 1))

    def twins(i):
        both_parts(i, twin_sem).wait_recv()

    send(0)
    xload_wait(1)
    send(1)
    pair_copy.start()
    wk_copy.start()
    wv_copy.start()

    def dot(a, b):
        return jnp.dot(a, b, preferred_element_type=F32)

    def dot_t(a, b):
        return lax.dot_general(a, b, (((0,), (0,)), ((), ())), preferred_element_type=F32)

    kbufs, vbufs = (kbuf0, kbuf1), (vbuf0, vbuf1)

    def project_q(c):
        q = dot(xbuf[c], wq[...]).astype(BF16)
        for h in range(nh):
            qt[h, :, c * tok:(c + 1) * tok] = q[:, h * HEAD:(h + 1) * HEAD].T

    def project(c, lo=0, hi=tok):
        xs = xbuf[c, lo:hi, :]
        kbufs[c % 2][lo:hi, :] = dot(xs, wk[...]).astype(BF16)
        vbufs[c % 2][lo:hi, :] = dot(xs, wv[...]).astype(BF16)

    def project_first(c):
        xs = xbuf[c, :, 0:cut]
        facc[:, 0:half] = dot(xs, wk[0:cut, :])
        facc[:, half:] = dot(xs, wv[0:cut, :])

    def project_second(c, lo, hi):
        xs = xbuf[c, lo:hi, cut:]
        kbufs[c % 2][lo:hi, :] = (facc[lo:hi, 0:half] + dot(xs, wk[cut:, :])).astype(BF16)
        vbufs[c % 2][lo:hi, :] = (facc[lo:hi, half:] + dot(xs, wv[cut:, :])).astype(BF16)

    def attend(c, heads=range(nh), last=False):
        kb, vb = kbufs[c % 2], vbufs[c % 2]

        for h in heads:
            sbuf[h] = dot(kb[:, h * HEAD:(h + 1) * HEAD], qt[h])
        for h in heads:
            s = sbuf[h]
            m_old = mrow[h]
            m_new = jnp.maximum(m_old, jnp.max(s, axis=0, keepdims=True))
            p = jnp.exp2((s - m_new) * scale)
            a = jnp.exp2((m_old - m_new) * scale)
            l_new = lrow[h] * a + jnp.sum(p, axis=0, keepdims=True)
            o_new = acc[h] * a + dot_t(vb[:, h * HEAD:(h + 1) * HEAD], p.astype(BF16))
            if not last:
                lrow[h] = l_new
                mrow[h] = m_new
                acc[h] = o_new
            else:
                o = (o_new * (1.0 / l_new)).astype(BF16)
                oown[h * HEAD:(h + 1) * HEAD, :] = o[:, 0:tok]
                osend[h * HEAD:(h + 1) * HEAD, :] = o[:, tok:]

    wq_copy.wait()
    project_q(0)
    wk_copy.wait()
    wv_copy.wait()
    wo_copy.start()
    project(0)
    pair_copy.wait_recv()
    project_q(1)
    project(1)
    arrive(0)
    attend(0)
    twins(0)
    project(2)
    arrive(1)
    attend(1)
    twins(1)
    project(3)
    attend(2)
    arrive(2)
    attend(3)
    twins(2)
    project(4)
    attend(4, range(0, 3))
    arrive(3)
    attend(4, range(3, 6))
    twins(3)
    project(5)
    attend(5)
    arrive(4)
    project(6, 0, tok // 2)
    twins(4)
    project(6, tok // 2, tok)
    arrive(5)
    attend(6)
    arrive(6)
    twins(5)
    project_first(7)
    project_second(7, 0, tok // 2)
    twins(6)
    project_second(7, tok // 2, tok)

    first = 3

    def ocopy(i):
        rows = slice(0, first * HEAD) if i == 0 else slice(first * HEAD, half)
        return remote(osend.at[rows, :], oother.at[rows, :], osend_sem, orecv_sem.at[i], partner)

    attend(7, range(0, first), last=True)
    ocopy(0).start()
    attend(7, range(first, nh), last=True)
    ocopy(1).start()
    wo_copy.wait()

    def wo_rows(start, n):
        return wo[pl.ds(pl.multiple_of(start, HEAD), n), :]

    cutrow = first * HEAD
    other = (1 - core) * half
    facc[...] = dot_t(oown[...], wo_rows(core * half, half))
    ocopy(0).wait_recv()
    facc[...] += dot_t(oother[0:cutrow, :], wo_rows(other, cutrow))
    ocopy(1).wait_recv()
    y_ref[...] = (facc[...] + dot_t(oother[cutrow:, :], wo_rows(other + cutrow, half - cutrow))).astype(BF16)

    sent = xbuf.at[0:7]
    remote(sent, sent, send_sem, pair_sem, partner).wait_send()
    remote(osend, osend, osend_sem, pair_sem, partner).wait_send()


def solution(mesh):
    def block(x, w_qkv, w_o):
        tok, width = x.shape[1], x.shape[2]
        half = width // 2
        nh = half // HEAD
        any_spec = pl.BlockSpec(memory_space=pl.ANY)
        dma = pltpu.SemaphoreType.DMA
        y = pl.pallas_call(
            kernel,
            out_shape=jax.ShapeDtypeStruct((tok, width), BF16),
            in_specs=[any_spec] * 3,
            out_specs=pl.BlockSpec(memory_space=pltpu.VMEM),
            scratch_shapes=[
                pltpu.VMEM((8, tok, width), BF16),
                pltpu.VMEM((width, half), BF16),
                pltpu.VMEM((width, half), BF16),
                pltpu.VMEM((width, half), BF16),
                pltpu.VMEM((width, width), BF16),
                pltpu.VMEM((nh, HEAD, 2 * tok), BF16),
                pltpu.VMEM((tok, half), BF16),
                pltpu.VMEM((tok, half), BF16),
                pltpu.VMEM((tok, half), BF16),
                pltpu.VMEM((tok, half), BF16),
                pltpu.VMEM((nh, HEAD, 2 * tok), F32),
                pltpu.VMEM((nh, 1, 2 * tok), F32),
                pltpu.VMEM((nh, 1, 2 * tok), F32),
                pltpu.VMEM((half, tok), BF16),
                pltpu.VMEM((half, tok), BF16),
                pltpu.VMEM((half, tok), BF16),
                pltpu.VMEM((tok, width), F32),
                pltpu.VMEM((nh, tok, 2 * tok), F32),
                dma((4,)), dma((2,)), dma(()), dma(()), dma(()), dma((7,)), dma((7,)), dma((2,)),
            ],
            compiler_params=pltpu.CompilerParams(
                collective_id=0, has_side_effects=True, vmem_limit_bytes=53 * 1024 * 1024),
            name="gather_attend",
        )(x[0], w_qkv, w_o.reshape(width, width))
        return y[None]

    return jax.shard_map(
        block, mesh=mesh,
        in_specs=(P("dp", ("cx", "cy"), None), P(None, None), P(None, None, None)),
        out_specs=P("dp", ("cx", "cy"), None), check_vma=False)
```

```python
import math

import jax
import jax.numpy as jnp
from jax import lax
from jax.experimental import pallas as pl
from jax.experimental.pallas import tpu as pltpu
from jax.sharding import PartitionSpec as P

MESH = pl.DeviceIdType.MESH
BF16, F32 = jnp.bfloat16, jnp.float32
HEAD = 128


def kernel(x_hbm, wqkv_hbm, wo_hbm, y_ref,
           xbuf, wq, wk, wv, wo, qt, kbuf0, kbuf1, vbuf0, vbuf1, acc, mrow, lrow, osend, oown, oother, facc, sbuf,
           w_sem, x_sem, pair_sem, send_sem, osend_sem, link_sem, twin_sem, orecv_sem):
    tok, width = x_hbm.shape
    half = width // 2
    nh = half // HEAD
    quarter = tok // 4
    cut = 8 * HEAD
    scale = math.log2(math.e) / math.sqrt(HEAD)

    dp, cx, cy = lax.axis_index("dp"), lax.axis_index("cx"), lax.axis_index("cy")
    core = lax.rem(cy, 2)
    partner = (dp, cx, cy + 1 - 2 * core)
    xnbr = (dp, cx, lax.rem(cy + 2, 4))
    ynbr = (dp, 1 - cx, cy)

    def wcopy(i, dst):
        cols = pl.ds(pl.multiple_of(i * width + core * half, HEAD), half)
        return pltpu.make_async_copy(wqkv_hbm.at[:, cols], dst, w_sem.at[i])

    wq_copy, wk_copy, wv_copy = wcopy(0, wq), wcopy(1, wk), wcopy(2, wv)
    wo_copy = pltpu.make_async_copy(wo_hbm, wo, w_sem.at[3])

    def own_rows(i, n=1):
        return xbuf.at[0, pl.ds(i * quarter, n * quarter), :]

    for i in (2, 0, 3, 1):
        pltpu.make_async_copy(x_hbm.at[pl.ds(i * quarter, quarter), :], own_rows(i), x_sem.at[i % 2]).start()

    def xload_wait(i):
        pltpu.make_async_copy(x_hbm.at[pl.ds(0, 2 * quarter), :], own_rows(0, 2), x_sem.at[i]).wait()

    barrier = pltpu.get_barrier_semaphore()
    for nbr in (partner, xnbr, ynbr):
        pl.semaphore_signal(barrier, inc=1, device_id=nbr, device_id_type=MESH)
    acc[...] = jnp.zeros_like(acc)
    lrow[...] = jnp.zeros_like(lrow)
    mrow[...] = jnp.full(mrow.shape, -jnp.inf, F32)
    wq_copy.start()
    xload_wait(0)
    pl.semaphore_wait(barrier, 3)

    pieces = [(c, slice(0, width)) for c in range(2, 7)] + [(7, slice(0, cut)), (7, slice(cut, width))]

    def part(c, q, cols):
        return xbuf.at[c, q * quarter:(q + 1) * quarter, cols]

    def remote(src, dst, ssem, rsem, dev):
        return pltpu.make_async_remote_copy(src_ref=src, dst_ref=dst, send_sem=ssem, recv_sem=rsem,
                                            device_id=dev, device_id_type=MESH)

    def link_copy(i, q):
        c, cols = pieces[i]
        dev = xnbr if q == 0 else ynbr
        if c < 6:
            src = own_rows((c if q == 0 else c - 2) % 4)
        else:
            src = part(c - 4, 1 - q, cols)
        return remote(src, part(c, q, cols), send_sem, link_sem.at[i], dev)

    def twin_copy(i, q):
        c, cols = pieces[i]
        return remote(part(c, q, cols), part(c, q + 2, cols), send_sem, twin_sem.at[i], partner)

    pair_copy = remote(xbuf.at[0], xbuf.at[1], send_sem, pair_sem, partner)
    depth = 3

    def send(i):
        if i < len(pieces):
            link_copy(i, 0).start()
            link_copy(i, 1).start()

    def both_parts(i, sems):
        c, cols = pieces[i]
        both = xbuf.at[c, 0:2 * quarter, cols]
        return remote(both, both, send_sem, sems.at[i], partner)

    def arrive(i):
        both_parts(i, link_sem).wait_recv()
        twin_copy(i, 0).start()
        twin_copy(i, 1).start()
        if i == 1:
            send(i + 2)
        send(i + depth - (i < 1))

    def twins(i):
        both_parts(i, twin_sem).wait_recv()

    send(0)
    xload_wait(1)
    send(1)
    pair_copy.start()
    wk_copy.start()
    wv_copy.start()

    def dot(a, b):
        return jnp.dot(a, b, preferred_element_type=F32)

    def dot_t(a, b):
        return lax.dot_general(a, b, (((0,), (0,)), ((), ())), preferred_element_type=F32)

    kbufs, vbufs = (kbuf0, kbuf1), (vbuf0, vbuf1)

    def project_q(c):
        q = dot(xbuf[c], wq[...]).astype(BF16)
        for h in range(nh):
            qt[h, :, c * tok:(c + 1) * tok] = q[:, h * HEAD:(h + 1) * HEAD].T

    def project(c, lo=0, hi=tok):
        xs = xbuf[c, lo:hi, :]
        kbufs[c % 2][lo:hi, :] = dot(xs, wk[...]).astype(BF16)
        vbufs[c % 2][lo:hi, :] = dot(xs, wv[...]).astype(BF16)

    def project_first(c):
        xs = xbuf[c, :, 0:cut]
        facc[:, 0:half] = dot(xs, wk[0:cut, :])
        facc[:, half:] = dot(xs, wv[0:cut, :])

    def project_second(c, lo, hi):
        xs = xbuf[c, lo:hi, cut:]
        kbufs[c % 2][lo:hi, :] = (facc[lo:hi, 0:half] + dot(xs, wk[cut:, :])).astype(BF16)
        vbufs[c % 2][lo:hi, :] = (facc[lo:hi, half:] + dot(xs, wv[cut:, :])).astype(BF16)

    def attend(c, heads=range(nh), last=False):
        kb, vb = kbufs[c % 2], vbufs[c % 2]

        for h in heads:
            sbuf[h] = dot(kb[:, h * HEAD:(h + 1) * HEAD], qt[h])
        for h in heads:
            s = sbuf[h]
            m_old = mrow[h]
            m_new = jnp.maximum(m_old, jnp.max(s, axis=0, keepdims=True))
            p = jnp.exp2((s - m_new) * scale)
            a = jnp.exp2((m_old - m_new) * scale)
            l_new = lrow[h] * a + jnp.sum(p, axis=0, keepdims=True)
            o_new = acc[h] * a + dot_t(vb[:, h * HEAD:(h + 1) * HEAD], p.astype(BF16))
            if not last:
                lrow[h] = l_new
                mrow[h] = m_new
                acc[h] = o_new
            else:
                o = (o_new * (1.0 / l_new)).astype(BF16)
                oown[h * HEAD:(h + 1) * HEAD, :] = o[:, 0:tok]
                osend[h * HEAD:(h + 1) * HEAD, :] = o[:, tok:]

    wq_copy.wait()
    project_q(0)
    wk_copy.wait()
    wv_copy.wait()
    wo_copy.start()
    project(0)
    pair_copy.wait_recv()
    project_q(1)
    project(1)
    arrive(0)
    attend(0)
    twins(0)
    project(2)
    arrive(1)
    attend(1)
    twins(1)
    project(3)
    attend(2)
    arrive(2)
    attend(3)
    twins(2)
    project(4)
    attend(4, range(0, 4))
    arrive(3)
    attend(4, range(4, 6))
    twins(3)
    project(5)
    attend(5)
    arrive(4)
    project(6, 0, tok // 2)
    twins(4)
    project(6, tok // 2, tok)
    arrive(5)
    attend(6)
    arrive(6)
    twins(5)
    project_first(7)
    project_second(7, 0, tok // 2)
    twins(6)
    project_second(7, tok // 2, tok)

    first = 4

    def ocopy(i):
        rows = slice(0, first * HEAD) if i == 0 else slice(first * HEAD, half)
        return remote(osend.at[rows, :], oother.at[rows, :], osend_sem, orecv_sem.at[i], partner)

    attend(7, range(0, first), last=True)
    ocopy(0).start()
    attend(7, range(first, nh), last=True)
    ocopy(1).start()
    wo_copy.wait()

    def wo_rows(start, n):
        return wo[pl.ds(pl.multiple_of(start, HEAD), n), :]

    cutrow = first * HEAD
    other = (1 - core) * half
    facc[...] = dot_t(oown[...], wo_rows(core * half, half))
    ocopy(0).wait_recv()
    facc[...] += dot_t(oother[0:cutrow, :], wo_rows(other, cutrow))
    ocopy(1).wait_recv()
    y_ref[...] = (facc[...] + dot_t(oother[cutrow:, :], wo_rows(other + cutrow, half - cutrow))).astype(BF16)

    sent = xbuf.at[0:7]
    remote(sent, sent, send_sem, pair_sem, partner).wait_send()
    remote(osend, osend, osend_sem, pair_sem, partner).wait_send()


def solution(mesh):
    def block(x, w_qkv, w_o):
        tok, width = x.shape[1], x.shape[2]
        half = width // 2
        nh = half // HEAD
        any_spec = pl.BlockSpec(memory_space=pl.ANY)
        dma = pltpu.SemaphoreType.DMA
        y = pl.pallas_call(
            kernel,
            out_shape=jax.ShapeDtypeStruct((tok, width), BF16),
            in_specs=[any_spec] * 3,
            out_specs=pl.BlockSpec(memory_space=pltpu.VMEM),
            scratch_shapes=[
                pltpu.VMEM((8, tok, width), BF16),
                pltpu.VMEM((width, half), BF16),
                pltpu.VMEM((width, half), BF16),
                pltpu.VMEM((width, half), BF16),
                pltpu.VMEM((width, width), BF16),
                pltpu.VMEM((nh, HEAD, 2 * tok), BF16),
                pltpu.VMEM((tok, half), BF16),
                pltpu.VMEM((tok, half), BF16),
                pltpu.VMEM((tok, half), BF16),
                pltpu.VMEM((tok, half), BF16),
                pltpu.VMEM((nh, HEAD, 2 * tok), F32),
                pltpu.VMEM((nh, 1, 2 * tok), F32),
                pltpu.VMEM((nh, 1, 2 * tok), F32),
                pltpu.VMEM((half, tok), BF16),
                pltpu.VMEM((half, tok), BF16),
                pltpu.VMEM((half, tok), BF16),
                pltpu.VMEM((tok, width), F32),
                pltpu.VMEM((nh, tok, 2 * tok), F32),
                dma((4,)), dma((2,)), dma(()), dma(()), dma(()), dma((7,)), dma((7,)), dma((2,)),
            ],
            compiler_params=pltpu.CompilerParams(
                collective_id=0, has_side_effects=True, vmem_limit_bytes=53 * 1024 * 1024),
            name="gather_attend",
        )(x[0], w_qkv, w_o.reshape(width, width))
        return y[None]

    return jax.shard_map(
        block, mesh=mesh,
        in_specs=(P("dp", ("cx", "cy"), None), P(None, None), P(None, None, None)),
        out_specs=P("dp", ("cx", "cy"), None), check_vma=False)
```
